256 devices in a mesh: dp: 128 (over z, y_lo, x, core), mp: 2 (over y_hi).
Axes of the slice: x: 4, y: 4 (y_hi: 2, y_lo: 2; y = y_hi * 2 + y_lo), z: 8, core: 2. Of those that a mesh axis runs over, the one named last changes fastest.
Arguments:
- context: bfloat16 [40960, 2048], P('dp', 'mp'), may hold values from -24 to 24
- out_weight: bfloat16 [2048, 3584], P('mp'), may hold values from -0.125 to 0.125
- cotangent: bfloat16 [40960, 3584], P('dp'), may hold values from -0.059814453 to 0.059814453
- norm_gain: float32 [3584], replicated, may hold values from 0.5 to 1.5
- first_moment: float32 [2, 1024, 3584], P('mp', 'dp'), may hold values from -6 to 6
- second_moment: float32 [2, 1024, 3584], P('mp', 'dp'), may hold values from 0.01 to 1
Outputs:
- new_weight: bfloat16 [2, 1024, 3584], P('mp', 'dp')
- new_first: float32 [2, 1024, 3584], P('mp', 'dp')
- new_second: float32 [2, 1024, 3584], P('mp', 'dp')
- grad_gain: float32 [3584], replicated
- grad_context: bfloat16 [40960, 2048], P('dp', 'mp')
The draws below stay inside these ranges and needn't reach their ends.
All inputs are finite; a program needn't handle non-finite values.
Results may differ from the reference program's by a relative error of at most 0.005.
Values may be sent and summed in bfloat16 or wider, within the bound.
A program may use at most 128 MiB of HBM per device.

```python
import math
import jax
import jax.numpy as jnp
from jax import lax

D = 3584
HQ = 2048
TOKENS = 40960
N_MP = 2


def with_spikes(result, own_key, source, target, parts, factor):
    def block_of(position):
        return (jnp.arange(result.shape[position]) // (result.shape[position] // parts)).reshape((-1,) + (1,) * (result.ndim - 1 - position))

    one_side = jax.random.permutation(own_key, parts)[block_of(target)]
    second = (block_of(target) + parts // 2) % parts
    return jnp.where((block_of(source) == one_side) | (block_of(source) == second), factor * result, result)


def shard_levels(stream_key, extent, split, least, high):
    gain, own = 1.0, jax.random.fold_in(stream_key, 6)
    for position, blocks in split:
        steps = jnp.exp(jax.random.uniform(jax.random.fold_in(own, position), (blocks,), jnp.float32, least / len(split), high / len(split)))
        gain = gain * jnp.repeat(steps, extent[position] // blocks).reshape([-1 if axis == position else 1 for axis in range(len(extent))])
    return gain


def centred(key, extent, spread, reach, pieces=(), dtype=jnp.bfloat16):
    gain = shard_levels(key, extent, pieces, -0.22, 0.18) if pieces else 1.0
    entries = jax.random.normal(key, extent, jnp.float32) * spread * gain
    return jnp.minimum(jnp.maximum(entries, -reach), reach).astype(dtype)


def gaussian_with(own_key, shape, width, limit, cuts, heavy, held_as=jnp.bfloat16):
    array = width * jax.random.normal(own_key, shape, jnp.float32)
    if cuts:
        array = array * shard_levels(own_key, shape, cuts, -0.22, 0.18)
    return jnp.clip(with_spikes(array, jax.random.fold_in(own_key, 3), *heavy), -limit, limit).astype(held_as)


def setup_inputs(seed: int = 0) -> dict:
    arg_keys = jax.random.split(jax.random.key(seed), 7)
    return {
        "context": gaussian_with(arg_keys[0], (TOKENS, HQ), 1.0, 24.0, ((0, 128), (1, 2)), (0, 1, 128, 5.5)),
        "out_weight": centred(arg_keys[1], (HQ, D), HQ ** -0.5, 0.125, ((0, 2),)),
        "cotangent": centred(arg_keys[2], (TOKENS, D), 0.01, 0.059814453, ((0, 128),)),
        "norm_gain": jnp.clip(1.0 + 0.1 * jax.random.normal(arg_keys[3], (D,), jnp.float32), 0.5, 1.5),
        "first_moment": centred(arg_keys[4], (N_MP, HQ // N_MP, D), 1.0, 6.0, ((0, 2), (1, 128)), jnp.float32),
        "second_moment": jnp.clip(jnp.exp(math.log(1.0) - 4.6051702 * jax.random.uniform(arg_keys[5], (N_MP, HQ // N_MP, D), jnp.float32) ** shard_levels(arg_keys[5], (N_MP, HQ // N_MP, D), ((0, 2), (1, 128)), -0.2, 0.2)), 0.01, 1.0),
    }


norm_floor = 0.1
learn_rate = 0.01
beta_one = 0.9
beta_two = 0.95
adam_floor = 1e-08

def reference(context, out_weight, cotangent, norm_gain, first_moment, second_moment):
    attn = jnp.dot(context, out_weight, preferred_element_type=jnp.float32)
    inverse = lax.rsqrt(lax.optimization_barrier(jnp.mean(attn * attn, axis=-1, keepdims=True)) + norm_floor)
    normed = attn * inverse
    upstream = cotangent.astype(jnp.float32)
    scaled = upstream * norm_gain
    grad_gain = lax.optimization_barrier(jnp.sum(upstream * normed, axis=0))
    grad_attn = (inverse * (scaled - normed * lax.optimization_barrier(jnp.mean(scaled * normed, axis=-1, keepdims=True)))).astype(jnp.bfloat16)
    grad_context = jnp.dot(grad_attn, out_weight.T, preferred_element_type=jnp.float32).astype(jnp.bfloat16)
    grad_weight = jnp.dot(context.T, grad_attn, preferred_element_type=jnp.float32)
    grad_weight = grad_weight.reshape(N_MP, HQ // N_MP, D)
    new_first = beta_one * first_moment + (1.0 - beta_one) * grad_weight
    new_second = beta_two * second_moment + (1.0 - beta_two) * grad_weight * grad_weight
    master = out_weight.astype(jnp.float32).reshape(N_MP, HQ // N_MP, D)
    new_weight = (master - learn_rate * new_first / (jnp.sqrt(new_second) + adam_floor)).astype(jnp.bfloat16)
    return (new_weight, new_first, new_second, grad_gain, grad_context)
```

```python
import functools

import jax
import jax.numpy as jnp
from jax import lax
from jax.experimental import pallas as pl
from jax.experimental.pallas import tpu as pltpu
from jax.sharding import Mesh
from jax.sharding import PartitionSpec as P

DP = ("dp_0", "dp_1", "dp_2", "dp_3")
MESH = pl.DeviceIdType.MESH
F32 = jnp.float32
BF16 = jnp.bfloat16

norm_floor = 0.1
learn_rate = 0.01
beta_one = 0.9
beta_two = 0.95
adam_floor = 1e-08

QR = 256


def dot_nn(a, b):
    return lax.dot_general(a, b, (((1,), (0,)), ((), ())), preferred_element_type=F32)


def dot_tn(a, b):
    return lax.dot_general(a, b, (((0,), (0,)), ((), ())), preferred_element_type=F32)


def dot_nt(a, b):
    return lax.dot_general(a, b, (((1,), (1,)), ((), ())), preferred_element_type=F32)


def send(src, dst, send_sem, recv_sem, axis, peer):
    return pltpu.make_async_remote_copy(
        src_ref=src,
        dst_ref=dst,
        send_sem=send_sem,
        recv_sem=recv_sem,
        device_id={axis: peer},
        device_id_type=MESH,
    )


def kernel(
    dims,
    ctx_hbm, w_hbm, cot_hbm, gain_ref, m1_hbm, m2_hbm,
    nw_ref, n1_ref, n2_ref, gg_ref, gc_ref,
    ctx_o, ctx_s, wv, cot, att, psend, precv, ssr, spr, gaf, gas,
    grad, r1, r2, zs, zr, yt, yr, fs, gr, m1v, m2v, gz, gx, gy, gm, gk,
    ld_w, ld, c_sem, p_s, p_r, ga_s, ga_r, sa_s, sa_r, x1_s, x1_r, x2_s, x2_r,
    z_s, z_r, y_s, y_r, f_sem, gz_s, gz_r, gx_s, gx_r, gt_s, gt_r,
):
    NZ, NY, NX, TH, H, D, NB, CB = dims
    NB2 = 2 * NB
    ZY = NZ * NY
    HZ = ZY // 2
    T = 2 * TH
    z = lax.axis_index("dp_0")
    yl = lax.axis_index("dp_1")
    x = lax.axis_index("dp_2")
    c = lax.axis_index("dp_3")
    m = lax.axis_index("mp")

    def away(me, d, n):
        return lax.rem(me + d, n)

    right, left, across = away(x, 1, NX), away(x, NX - 1, NX), away(x, 2, NX)
    om, oc, oy = 1 - m, 1 - c, 1 - yl

    def each_block(n, body):
        def step(i, carry):
            body(i)
            return carry

        lax.fori_loop(0, n, step, 0)

    ctx_loads = [
        pltpu.make_async_copy(ctx_hbm.at[pl.ds(k * TH, TH), :], ctx_o.at[k], ld.at[k]) for k in range(2)
    ]
    cot_load = pltpu.make_async_copy(
        cot_hbm.at[pl.ds(pl.multiple_of(m * TH, TH), TH), :], cot, ld.at[2]
    )
    m1_load = pltpu.make_async_copy(m1_hbm, m1v, ld.at[3])
    m2_load = pltpu.make_async_copy(m2_hbm, m2v, ld.at[4])

    def w_load(b):
        return pltpu.make_async_copy(
            w_hbm.at[:, pl.ds(pl.multiple_of(b * CB, CB), CB)], wv.at[b], ld_w.at[b]
        )

    for copy in ctx_loads:
        copy.start()
    each_block(NB2, lambda b: w_load(b).start())
    cot_load.start()
    m1_load.start()
    m2_load.start()

    barrier = pltpu.get_barrier_semaphore()
    peers = [("dp_3", oc), ("mp", om), ("dp_1", oy)]
    peers += [("dp_2", away(x, d, NX)) for d in range(1, NX)]
    peers += [("dp_0", away(z, d, NZ)) for d in range(1, NZ)]
    for axis, peer in peers:
        pl.semaphore_signal(barrier, inc=1, device_id={axis: peer}, device_id_type=MESH)
    pl.semaphore_wait(barrier, len(peers))

    for copy in ctx_loads:
        copy.wait()

    def ctx_swap():
        return send(ctx_o, ctx_s, c_sem.at[0], c_sem.at[1], "dp_3", oc)

    ctx_swap().start()

    def partial_send(b):
        return send(psend.at[b], precv.at[b], p_s.at[b], p_r.at[b], "mp", om)

    def project_theirs(b):
        w_load(b).wait()
        psend[b] = dot_nn(ctx_o[om], wv[b]).astype(BF16)
        partial_send(b).start()

    each_block(NB2, project_theirs)

    cot_load.wait()
    ssr[...] = jnp.zeros_like(ssr)
    spr[...] = jnp.zeros_like(spr)
    gz[z] = jnp.zeros(gz.shape[1:], F32)

    def columns(b):
        return pl.ds(pl.multiple_of(b * CB, CB), CB)

    def project_ours(b):
        att[b] = dot_nn(ctx_o[m], wv[b])

    each_block(NB2, project_ours)

    def add_theirs(b):
        partial_send(b).wait_recv()
        a = att[b] + precv[b].astype(F32)
        att[b] = a
        s = cot[:, columns(b)].astype(F32) * gain_ref[:, columns(b)]
        sq, pr = a * a, a * s
        for k in range(CB // 128):
            ssr[...] += sq[:, k * 128 : (k + 1) * 128]
            spr[...] += pr[:, k * 128 : (k + 1) * 128]

    each_block(NB2, add_theirs)

    inverse = lax.rsqrt(jnp.sum(ssr[...], axis=1, keepdims=True) / D + norm_floor)
    mean_sn = inverse * (jnp.sum(spr[...], axis=1, keepdims=True) / D)

    def ga_send(h, j):
        return send(gaf.at[h, j, m], gaf.at[h, j, m], ga_s.at[h, j], ga_r.at[h, j], "mp", om)

    def ga_wait(h, j):
        return send(gaf.at[h, j, om], gaf.at[h, j, om], ga_s.at[h, j], ga_r.at[h, j], "mp", om)

    def side_send(j, k, who):
        return send(gaf.at[oc, j, who], gas.at[j, who], sa_s.at[j, k], sa_r.at[j, k], "dp_3", oc)

    def side_wait(j, k, who):
        return send(gas.at[j, who], gas.at[j, who], sa_s.at[j, k], sa_r.at[j, k], "dp_3", oc)

    def norm_gradient(j):
        for h in range(2):
            b = h * NB + j
            a = att[b]
            u = cot[:, columns(b)].astype(F32)
            s = u * gain_ref[:, columns(b)]
            normed = a * inverse
            gaf[h, j, m] = (inverse * (s - normed * mean_sn)).astype(BF16)
            ga_send(h, j).start()
            gz[z, pl.ds(b, 1), :] = jnp.sum(u * normed, axis=0, keepdims=True)
        side_send(j, 0, m).start()

    each_block(NB, norm_gradient)

    def gain_hop(buf, axis, me, n, ss, rs):
        return [
            send(buf.at[me], buf.at[me], ss.at[d], rs.at[d], axis, away(me, d, n)) for d in range(1, n)
        ]

    def gain_wait(buf, axis, me, n, ss, rs):
        for d in range(1, n):
            src = away(me, n - d, n)
            send(buf.at[src], buf.at[src], ss.at[d], rs.at[d], axis, src).wait_recv()

    hops = [
        (gz, "dp_0", z, NZ, gz_s, gz_r),
        (gx, "dp_2", x, NX, gx_s, gx_r),
        (gy, "dp_1", yl, NY, gt_s.at[0], gt_r.at[0]),
        (gm, "mp", m, 2, gt_s.at[1], gt_r.at[1]),
        (gk, "dp_3", c, 2, gt_s.at[2], gt_r.at[2]),
    ]

    def summed(buf, n):
        total = buf[0]
        for i in range(1, n):
            total = total + buf[i]
        return total

    for copy in gain_hop(*hops[0]):
        copy.start()

    def gain_stage(k):
        buf, _, _, n, _, _ = hops[k]
        gain_wait(*hops[k])
        total = summed(buf, n)
        if k + 1 < len(hops):
            nxt = hops[k + 1]
            nxt[0][nxt[2]] = total
            for copy in gain_hop(*nxt):
                copy.start()
        else:
            for b in range(NB2):
                gg_ref[:, b * CB : (b + 1) * CB] = total[b : b + 1, :]

    ctx_swap().wait_recv()

    def gather_grad_attn(j):
        ga_wait(0, j).wait_recv()
        ga_wait(1, j).wait_recv()
        side_send(j, 1, om).start()

    def x1_send(j, k):
        part = pl.ds(k * HZ, HZ)
        return send(
            grad.at[j, across, part], r1.at[j, k], x1_s.at[j, k], x1_r.at[j, k], "dp_2", right if k == 0 else left
        )

    def x2_send(j, k):
        peer = right if k == 0 else left
        return send(grad.at[j, peer], r2.at[j, k], x2_s.at[j, k], x2_r.at[j, k], "dp_2", peer)

    def z_send(j, d):
        peer = away(z, d, NZ)
        return send(zs.at[j, peer], zr.at[j, d], z_s.at[j, d], z_r.at[j, d], "dp_0", peer)

    def y_send(j):
        return send(yt.at[j, oy], yr.at[j], y_s.at[j], y_r.at[j], "dp_1", oy)

    def weight_grad(j):
        side_wait(j, 0, m).wait_recv()
        side_wait(j, 1, om).wait_recv()
        ours = gaf[c, j].reshape(T, CB)
        theirs = gas[j].reshape(T, CB)
        per = QR // (NX * 16)
        for q in range(H // QR):
            cols = slice(q * QR, (q + 1) * QR)
            part = dot_tn(ctx_o[:, :, cols].reshape(T, QR), ours)
            part = part + dot_tn(ctx_s[:, :, cols].reshape(T, QR), theirs)
            part = part.reshape(per, NX, 16, CB).astype(BF16)
            for k in range(NX):
                grad[j, k, q * per : (q + 1) * per] = part[:, k]
        x1_send(j, 0).start()
        x1_send(j, 1).start()

    def x_first(j):
        x1_send(j, 0).wait_recv()
        x1_send(j, 1).wait_recv()
        grad[j, right, :HZ] = (grad[j, right, :HZ].astype(F32) + r1[j, 0].astype(F32)).astype(BF16)
        grad[j, left, HZ:] = (grad[j, left, HZ:].astype(F32) + r1[j, 1].astype(F32)).astype(BF16)
        x2_send(j, 0).start()
        x2_send(j, 1).start()

    def x_second(j):
        x2_send(j, 0).wait_recv()
        x2_send(j, 1).wait_recv()
        total = grad[j, x].astype(F32) + r2[j, 0].astype(F32) + r2[j, 1].astype(F32)
        zs[j] = total.astype(BF16).reshape(NZ, NY, 16, CB)
        for d in range(1, NZ):
            z_send(j, d).start()

    def z_sum(j):
        for d in range(1, NZ):
            z_send(j, d).wait_recv()
        total = zs[j, z].astype(F32)
        for d in range(1, NZ):
            total = total + zr[j, d].astype(F32)
        yt[j] = total
        y_send(j).start()

    def context_grad(k):
        rows = pl.ds(pl.multiple_of(k * QR, QR), QR)
        total = None
        for h in range(2):
            for j in range(NB):
                term = dot_nt(gaf[h, j].reshape(T, CB), wv[h * NB + j, rows, :])
                total = term if total is None else total + term
        gc_ref[:, rows] = total.astype(BF16)

    stages = [z_sum, x_second, x_first, weight_grad, gather_grad_attn]

    def step(t):
        for depth, stage in enumerate(stages):
            lag = len(stages) - 1 - depth

            @pl.when((t >= lag) & (t < NB + lag))
            def _():
                stage(t - lag)

        for k in range(len(hops)):

            @pl.when(t == k + 1)
            def _():
                gain_stage(k)

        @pl.when((t >= NB) & (t < NB + H // QR))
        def _():
            context_grad(t - NB)

    each_block(NB + max(len(stages) - 1, len(hops), H // QR), step)

    def finish(j):
        y_send(j).wait_recv()
        total = yt[j, yl] + yr[j]
        fs[0, j] = total[:8]
        fs[1, j] = total[8:]

    each_block(NB, finish)

    def core_swap():
        return send(fs.at[oc], gr.at[c], f_sem.at[0], f_sem.at[1], "dp_3", oc)

    core_swap().start()
    gr[c] = fs[c]
    m1_load.wait()
    m2_load.wait()
    send(gr.at[oc], gr.at[oc], f_sem.at[0], f_sem.at[1], "dp_3", oc).wait_recv()
    row = pl.multiple_of(((z * NY + yl) * NX + x) * 16, 16)
    for b in range(NB2):
        cols = slice(b * CB, (b + 1) * CB)
        g = gr[b // NB, b % NB]
        first = beta_one * m1v[:, cols] + (1.0 - beta_one) * g
        second = beta_two * m2v[:, cols] + (1.0 - beta_two) * g * g
        both = wv[b, pl.ds(row, 16), :].astype(F32)
        master = jnp.where(c == 0, both[:8], both[8:])
        n1_ref[:, cols] = first
        n2_ref[:, cols] = second
        nw_ref[:, cols] = (master - learn_rate * first / (jnp.sqrt(second) + adam_floor)).astype(BF16)

    ctx_swap().wait_send()
    core_swap().wait_send()
    each_block(NB2, lambda b: partial_send(b).wait_send())
    for hop in hops:
        for copy in gain_hop(*hop):
            copy.wait_send()

    def drain(j):
        for h in range(2):
            ga_send(h, j).wait_send()
            x1_send(j, h).wait_send()
            x2_send(j, h).wait_send()
        side_send(j, 0, m).wait_send()
        side_send(j, 1, om).wait_send()
        for d in range(1, NZ):
            z_send(j, d).wait_send()
        y_send(j).wait_send()

    each_block(NB, drain)


def per_device(sizes, block, context, out_weight, cotangent, norm_gain, first_moment, second_moment):
    NZ, NY, NX = sizes
    T, H = context.shape
    D = out_weight.shape[1]
    TH, CB = T // 2, block
    NB = D // (2 * CB)
    NB2 = 2 * NB
    ZY = NZ * NY
    rows8 = (NB2 + 7) // 8 * 8
    dims = (NZ, NY, NX, TH, H, D, NB, CB)
    dma = pltpu.SemaphoreType.DMA
    scratch = [
        pltpu.VMEM((2, TH, H), BF16),
        pltpu.VMEM((2, TH, H), BF16),
        pltpu.VMEM((NB2, H, CB), BF16),
        pltpu.VMEM((TH, D), BF16),
        pltpu.VMEM((NB2, TH, CB), F32),
        pltpu.VMEM((NB2, TH, CB), BF16),
        pltpu.VMEM((NB2, TH, CB), BF16),
        pltpu.VMEM((TH, 128), F32),
        pltpu.VMEM((TH, 128), F32),
        pltpu.VMEM((2, NB, 2, TH, CB), BF16),
        pltpu.VMEM((NB, 2, TH, CB), BF16),
        pltpu.VMEM((NB, NX, ZY, 16, CB), BF16),
        pltpu.VMEM((NB, 2, ZY // 2, 16, CB), BF16),
        pltpu.VMEM((NB, 2, ZY, 16, CB), BF16),
        pltpu.VMEM((NB, NZ, NY, 16, CB), BF16),
        pltpu.VMEM((NB, NZ, NY, 16, CB), BF16),
        pltpu.VMEM((NB, NY, 16, CB), F32),
        pltpu.VMEM((NB, 16, CB), F32),
        pltpu.VMEM((2, NB, 8, CB), F32),
        pltpu.VMEM((2, NB, 8, CB), F32),
        pltpu.VMEM((8, D), F32),
        pltpu.VMEM((8, D), F32),
        pltpu.VMEM((NZ, rows8, CB), F32),
        pltpu.VMEM((NX, rows8, CB), F32),
        pltpu.VMEM((NY, rows8, CB), F32),
        pltpu.VMEM((2, rows8, CB), F32),
        pltpu.VMEM((2, rows8, CB), F32),
        dma((NB2,)), dma((5,)), dma((2,)),
        dma((NB2,)), dma((NB2,)),
        dma((2, NB)), dma((2, NB)),
        dma((NB, 2)), dma((NB, 2)),
        dma((NB, 2)), dma((NB, 2)),
        dma((NB, 2)), dma((NB, 2)),
        dma((NB, NZ)), dma((NB, NZ)),
        dma((NB,)), dma((NB,)),
        dma((2,)),
        dma((NZ,)), dma((NZ,)),
        dma((NX,)), dma((NX,)),
        dma((3, 2)), dma((3, 2)),
    ]
    any_space = pl.BlockSpec(memory_space=pl.ANY)
    vmem = pl.BlockSpec(memory_space=pltpu.VMEM)
    nw, n1, n2, gg, gc = pl.pallas_call(
        functools.partial(kernel, dims),
        out_shape=[
            jax.ShapeDtypeStruct((8, D), BF16),
            jax.ShapeDtypeStruct((8, D), F32),
            jax.ShapeDtypeStruct((8, D), F32),
            jax.ShapeDtypeStruct((1, D), F32),
            jax.ShapeDtypeStruct((T, H), BF16),
        ],
        in_specs=[any_space, any_space, any_space, vmem, any_space, any_space],
        out_specs=[vmem] * 5,
        scratch_shapes=scratch,
        compiler_params=pltpu.CompilerParams(
            collective_id=0, has_side_effects=True, vmem_limit_bytes=60 * 1024 * 1024
        ),
        name="step",
    )(context, out_weight, cotangent, norm_gain.reshape(1, D), first_moment[0], second_moment[0])
    return (nw[None], n1[None], n2[None], gg.reshape(D), gc)


def build(finer, block):
    sizes = tuple(finer.shape[a] for a in ("dp_0", "dp_1", "dp_2"))
    placed = (P(DP, "mp"), P("mp", None), P(DP, None), P(), P("mp", DP, None), P("mp", DP, None))
    return jax.shard_map(
        functools.partial(per_device, sizes, block),
        mesh=finer,
        in_specs=placed,
        out_specs=(P("mp", DP, None), P("mp", DP, None), P("mp", DP, None), P(), P(DP, "mp")),
        check_vma=False,
    )


def solution(mesh):
    finer = Mesh(
        mesh.devices.reshape(8, 2, 4, 2, mesh.shape["mp"]), ("dp_0", "dp_1", "dp_2", "dp_3", "mp")
    )
    return build(finer, 256)
```

```python
import functools

import jax
import jax.numpy as jnp
from jax import lax
from jax.experimental import pallas as pl
from jax.experimental.pallas import tpu as pltpu
from jax.sharding import Mesh
from jax.sharding import PartitionSpec as P

DP = ("dp_0", "dp_1", "dp_2", "dp_3")
MESH = pl.DeviceIdType.MESH
F32 = jnp.float32
BF16 = jnp.bfloat16

norm_floor = 0.1
learn_rate = 0.01
beta_one = 0.9
beta_two = 0.95
adam_floor = 1e-08

QR = 256


def dot_nn(a, b):
    return lax.dot_general(a, b, (((1,), (0,)), ((), ())), preferred_element_type=F32)


def dot_tn(a, b):
    return lax.dot_general(a, b, (((0,), (0,)), ((), ())), preferred_element_type=F32)


def dot_nt(a, b):
    return lax.dot_general(a, b, (((1,), (1,)), ((), ())), preferred_element_type=F32)


def send(src, dst, send_sem, recv_sem, axis, peer):
    return pltpu.make_async_remote_copy(
        src_ref=src,
        dst_ref=dst,
        send_sem=send_sem,
        recv_sem=recv_sem,
        device_id={axis: peer},
        device_id_type=MESH,
    )


def kernel(
    dims,
    ctx_hbm, w_hbm, cot_hbm, gain_ref, m1_hbm, m2_hbm,
    nw_ref, n1_ref, n2_ref, gg_ref, gc_ref,
    ctx_o, ctx_s, wv, cot, att, psend, precv, ssr, spr, gaf, gas,
    grad, r1, r2, zs, zr, fs, gr, m1v, m2v, gz, gx, gy, gm, gk,
    ld_w, ld, c_sem, p_s, p_r, ga_s, ga_r, sa_s, sa_r, x1_s, x1_r, x2_s, x2_r,
    z_s, z_r, f_s, f_r, gz_s, gz_r, gx_s, gx_r, gt_s, gt_r,
):
    NZ, NY, NX, TH, H, D, NB, CB = dims
    NB2 = 2 * NB
    ZY = NZ * NY
    HZ = ZY // 2
    T = 2 * TH
    z = lax.axis_index("dp_0")
    yl = lax.axis_index("dp_1")
    x = lax.axis_index("dp_2")
    c = lax.axis_index("dp_3")
    m = lax.axis_index("mp")

    def away(me, d, n):
        return lax.rem(me + d, n)

    right, left, across = away(x, 1, NX), away(x, NX - 1, NX), away(x, 2, NX)
    om, oc = 1 - m, 1 - c
    owners = [(d, e) for d in range(NZ) for e in range(NY) if (d, e) != (0, 0)]

    def each_block(n, body):
        def step(i, carry):
            body(i)
            return carry

        lax.fori_loop(0, n, step, 0)

    ctx_loads = [
        pltpu.make_async_copy(ctx_hbm.at[pl.ds(k * TH, TH), :], ctx_o.at[k], ld.at[k]) for k in range(2)
    ]
    cot_load = pltpu.make_async_copy(
        cot_hbm.at[pl.ds(pl.multiple_of(m * TH, TH), TH), :], cot, ld.at[2]
    )
    m1_load = pltpu.make_async_copy(m1_hbm, m1v, ld.at[3])
    m2_load = pltpu.make_async_copy(m2_hbm, m2v, ld.at[4])

    def w_load(b):
        return pltpu.make_async_copy(
            w_hbm.at[:, pl.ds(pl.multiple_of(b * CB, CB), CB)], wv.at[b], ld_w.at[b]
        )

    for copy in ctx_loads:
        copy.start()
    each_block(NB2, lambda b: w_load(b).start())
    cot_load.start()
    m1_load.start()
    m2_load.start()

    barrier = pltpu.get_barrier_semaphore()
    peers = [{"dp_3": oc}, {"mp": om}]
    peers += [{"dp_2": away(x, d, NX)} for d in range(1, NX)]
    peers += [{"dp_0": away(z, d, NZ), "dp_1": away(yl, e, NY)} for d, e in owners]
    for peer in peers:
        pl.semaphore_signal(barrier, inc=1, device_id=peer, device_id_type=MESH)
    with jax.named_scope("greet"):
        pl.semaphore_wait(barrier, len(peers))

    with jax.named_scope("ctx_wait"):
        for copy in ctx_loads:
            copy.wait()

    def ctx_swap():
        return send(ctx_o, ctx_s, c_sem.at[0], c_sem.at[1], "dp_3", oc)

    ctx_swap().start()

    def partial_send(b):
        return send(psend.at[b], precv.at[b], p_s.at[b], p_r.at[b], "mp", om)

    def project_theirs(b):
        w_load(b).wait()
        psend[b] = dot_nn(ctx_o[om], wv[b]).astype(BF16)
        partial_send(b).start()

    with jax.named_scope("project_theirs"):
        each_block(NB2, project_theirs)

    cot_load.wait()
    ssr[...] = jnp.zeros_like(ssr)
    spr[...] = jnp.zeros_like(spr)
    gz[z] = jnp.zeros(gz.shape[1:], F32)

    def columns(b):
        return pl.ds(pl.multiple_of(b * CB, CB), CB)

    def project_ours(b):
        att[b] = dot_nn(ctx_o[m], wv[b])

    with jax.named_scope("project_ours"):
        each_block(NB2, project_ours)

    def add_theirs(b):
        with jax.named_scope("wait_partial"):
            partial_send(b).wait_recv()
        a = att[b] + precv[b].astype(F32)
        att[b] = a
        s = cot[:, columns(b)].astype(F32) * gain_ref[:, columns(b)]
        sq, pr = a * a, a * s
        for k in range(CB // 128):
            ssr[...] += sq[:, k * 128 : (k + 1) * 128]
            spr[...] += pr[:, k * 128 : (k + 1) * 128]

    with jax.named_scope("add_theirs"):
        each_block(NB2, add_theirs)

    inverse = lax.rsqrt(jnp.sum(ssr[...], axis=1, keepdims=True) / D + norm_floor)
    mean_sn = inverse * (jnp.sum(spr[...], axis=1, keepdims=True) / D)

    def ga_send(h, j):
        return send(gaf.at[h, j, m], gaf.at[h, j, m], ga_s.at[h, j], ga_r.at[h, j], "mp", om)

    def ga_wait(h, j):
        return send(gaf.at[h, j, om], gaf.at[h, j, om], ga_s.at[h, j], ga_r.at[h, j], "mp", om)

    def side_send(j, k, who):
        return send(gaf.at[oc, j, who], gas.at[j, who], sa_s.at[j, k], sa_r.at[j, k], "dp_3", oc)

    def side_wait(j, k, who):
        return send(gas.at[j, who], gas.at[j, who], sa_s.at[j, k], sa_r.at[j, k], "dp_3", oc)

    def norm_gradient(j):
        for h in range(2):
            b = h * NB + j
            a = att[b]
            u = cot[:, columns(b)].astype(F32)
            s = u * gain_ref[:, columns(b)]
            normed = a * inverse
            gaf[h, j, m] = (inverse * (s - normed * mean_sn)).astype(BF16)
            ga_send(h, j).start()
            gz[z, pl.ds(b, 1), :] = jnp.sum(u * normed, axis=0, keepdims=True)
        side_send(j, 0, m).start()

    with jax.named_scope("norm_gradient"):
        each_block(NB, norm_gradient)

    def gain_hop(buf, axis, me, n, ss, rs):
        return [
            send(buf.at[me], buf.at[me], ss.at[d], rs.at[d], axis, away(me, d, n)) for d in range(1, n)
        ]

    def gain_wait(buf, axis, me, n, ss, rs):
        for d in range(1, n):
            src = away(me, n - d, n)
            send(buf.at[src], buf.at[src], ss.at[d], rs.at[d], axis, src).wait_recv()

    hops = [
        (gz, "dp_0", z, NZ, gz_s, gz_r),
        (gx, "dp_2", x, NX, gx_s, gx_r),
        (gy, "dp_1", yl, NY, gt_s.at[0], gt_r.at[0]),
        (gm, "mp", m, 2, gt_s.at[1], gt_r.at[1]),
        (gk, "dp_3", c, 2, gt_s.at[2], gt_r.at[2]),
    ]

    def summed(buf, n):
        total = buf[0]
        for i in range(1, n):
            total = total + buf[i]
        return total

    for copy in gain_hop(*hops[0]):
        copy.start()

    def gain_stage(k):
        buf, _, _, n, _, _ = hops[k]
        gain_wait(*hops[k])
        total = summed(buf, n)
        if k + 1 < len(hops):
            nxt = hops[k + 1]
            nxt[0][nxt[2]] = total
            for copy in gain_hop(*nxt):
                copy.start()
        else:
            for b in range(NB2):
                gg_ref[:, b * CB : (b + 1) * CB] = total[b : b + 1, :]

    ctx_swap().wait_recv()

    def gather_grad_attn(j):
        ga_wait(0, j).wait_recv()
        ga_wait(1, j).wait_recv()
        side_send(j, 1, om).start()

    def x1_send(j, k):
        part = pl.ds(k * HZ, HZ)
        return send(
            grad.at[j, across, part], r1.at[j, k], x1_s.at[j, k], x1_r.at[j, k], "dp_2", right if k == 0 else left
        )

    def x2_send(j, k):
        peer = right if k == 0 else left
        return send(grad.at[j, peer], r2.at[j, k], x2_s.at[j, k], x2_r.at[j, k], "dp_2", peer)

    def z_send(j, d, e):
        zp, yp = away(z, d, NZ), away(yl, e, NY)
        return pltpu.make_async_remote_copy(
            src_ref=zs.at[j, zp, yp],
            dst_ref=zr.at[j, d, e],
            send_sem=z_s.at[j, d, e],
            recv_sem=z_r.at[j, d, e],
            device_id={"dp_0": zp, "dp_1": yp},
            device_id_type=MESH,
        )

    def core_send(j):
        return send(fs.at[oc, j], gr.at[c, j], f_s.at[j], f_r.at[j], "dp_3", oc)

    def core_wait(j):
        return send(gr.at[oc, j], gr.at[oc, j], f_s.at[j], f_r.at[j], "dp_3", oc)

    def weight_grad(j):
        side_wait(j, 0, m).wait_recv()
        side_wait(j, 1, om).wait_recv()
        ours = gaf[c, j].reshape(T, CB)
        theirs = gas[j].reshape(T, CB)
        per = QR // (NX * 16)
        for q in range(H // QR):
            cols = slice(q * QR, (q + 1) * QR)
            part = dot_tn(ctx_o[:, :, cols].reshape(T, QR), ours)
            part = part + dot_tn(ctx_s[:, :, cols].reshape(T, QR), theirs)
            part = part.reshape(per, NX, 16, CB).astype(BF16)
            for k in range(NX):
                grad[j, k, q * per : (q + 1) * per] = part[:, k]
        x1_send(j, 0).start()
        x1_send(j, 1).start()

    def x_first(j):
        x1_send(j, 0).wait_recv()
        x1_send(j, 1).wait_recv()
        grad[j, right, :HZ] = (grad[j, right, :HZ].astype(F32) + r1[j, 0].astype(F32)).astype(BF16)
        grad[j, left, HZ:] = (grad[j, left, HZ:].astype(F32) + r1[j, 1].astype(F32)).astype(BF16)
        x2_send(j, 0).start()
        x2_send(j, 1).start()

    def x_second(j):
        x2_send(j, 0).wait_recv()
        x2_send(j, 1).wait_recv()
        total = grad[j, x].astype(F32) + r2[j, 0].astype(F32) + r2[j, 1].astype(F32)
        zs[j] = total.astype(BF16).reshape(NZ, NY, 16, CB)
        for d, e in owners:
            z_send(j, d, e).start()

    def z_sum(j):
        for d, e in owners:
            z_send(j, d, e).wait_recv()
        total = zs[j, z, yl].astype(F32)
        for d, e in owners:
            total = total + zr[j, d, e].astype(F32)
        fs[0, j] = total[:8]
        fs[1, j] = total[8:]
        core_send(j).start()

    def context_grad(k):
        rows = pl.ds(pl.multiple_of(k * QR, QR), QR)
        total = None
        for h in range(2):
            for j in range(NB):
                term = dot_nt(gaf[h, j].reshape(T, CB), wv[h * NB + j, rows, :])
                total = term if total is None else total + term
        gc_ref[:, rows] = total.astype(BF16)

    stages = [(weight_grad, 1), (x_first, 2), (x_second, 4), (z_sum, 6), (gather_grad_attn, 0)]
    gain_steps = (2, 4, NB + 1, NB + 2, NB + 3)

    def step(t):
        for stage, lag in stages:

            @pl.when((t >= lag) & (t < NB + lag))
            def _():
                with jax.named_scope(stage.__name__):
                    stage(t - lag)

        for k, when in enumerate(gain_steps):

            @pl.when(t == when)
            def _():
                with jax.named_scope("gain_stage"):
                    gain_stage(k)

        @pl.when((t >= NB) & (t < NB + H // QR))
        def _():
            with jax.named_scope("context_grad"):
                context_grad(t - NB)

    each_block(NB + 6, step)

    gr[c] = fs[c]
    m1_load.wait()
    m2_load.wait()
    with jax.named_scope("core_wait"):
        each_block(NB, lambda j: core_wait(j).wait_recv())
    row = pl.multiple_of(((z * NY + yl) * NX + x) * 16, 16)
    for b in range(NB2):
        cols = slice(b * CB, (b + 1) * CB)
        g = gr[b // NB, b % NB]
        first = beta_one * m1v[:, cols] + (1.0 - beta_one) * g
        second = beta_two * m2v[:, cols] + (1.0 - beta_two) * g * g
        both = wv[b, pl.ds(row, 16), :].astype(F32)
        master = jnp.where(c == 0, both[:8], both[8:])
        n1_ref[:, cols] = first
        n2_ref[:, cols] = second
        nw_ref[:, cols] = (master - learn_rate * first / (jnp.sqrt(second) + adam_floor)).astype(BF16)

    ctx_swap().wait_send()
    each_block(NB2, lambda b: partial_send(b).wait_send())
    for hop in hops:
        for copy in gain_hop(*hop):
            copy.wait_send()

    def drain(j):
        for h in range(2):
            ga_send(h, j).wait_send()
            x1_send(j, h).wait_send()
            x2_send(j, h).wait_send()
        side_send(j, 0, m).wait_send()
        side_send(j, 1, om).wait_send()
        for d, e in owners:
            z_send(j, d, e).wait_send()
        core_send(j).wait_send()

    with jax.named_scope("drain"):
        each_block(NB, drain)


def deliver(*refs):
    n = (len(refs) - 1) // 3
    src, dst, held, sem = refs[:n], refs[n : 2 * n], refs[2 * n : 3 * n], refs[-1]
    into = [pltpu.make_async_copy(s, h, sem.at[i]) for i, (s, h) in enumerate(zip(src, held))]
    out = [pltpu.make_async_copy(h, d, sem.at[n + i]) for i, (h, d) in enumerate(zip(held, dst))]
    for copy in into:
        copy.start()
    for first, second in zip(into, out):
        first.wait()
        second.start()
    for copy in out:
        copy.wait()


def delivered(arrays):
    space = pl.BlockSpec(memory_space=pl.ANY)
    return pl.pallas_call(
        deliver,
        out_shape=[jax.ShapeDtypeStruct(a.shape, a.dtype) for a in arrays],
        in_specs=[space] * len(arrays),
        out_specs=[space] * len(arrays),
        scratch_shapes=[pltpu.VMEM(a.shape, a.dtype) for a in arrays]
        + [pltpu.SemaphoreType.DMA((2 * len(arrays),))],
        name="deliver",
    )(*arrays)


def per_device(sizes, block, context, out_weight, cotangent, norm_gain, first_moment, second_moment):
    NZ, NY, NX = sizes
    T, H = context.shape
    D = out_weight.shape[1]
    TH, CB = T // 2, block
    NB = D // (2 * CB)
    NB2 = 2 * NB
    ZY = NZ * NY
    rows8 = (NB2 + 7) // 8 * 8
    dims = (NZ, NY, NX, TH, H, D, NB, CB)
    dma = pltpu.SemaphoreType.DMA
    scratch = [
        pltpu.VMEM((2, TH, H), BF16),
        pltpu.VMEM((2, TH, H), BF16),
        pltpu.VMEM((NB2, H, CB), BF16),
        pltpu.VMEM((TH, D), BF16),
        pltpu.VMEM((NB2, TH, CB), F32),
        pltpu.VMEM((NB2, TH, CB), BF16),
        pltpu.VMEM((NB2, TH, CB), BF16),
        pltpu.VMEM((TH, 128), F32),
        pltpu.VMEM((TH, 128), F32),
        pltpu.VMEM((2, NB, 2, TH, CB), BF16),
        pltpu.VMEM((NB, 2, TH, CB), BF16),
        pltpu.VMEM((NB, NX, ZY, 16, CB), BF16),
        pltpu.VMEM((NB, 2, ZY // 2, 16, CB), BF16),
        pltpu.VMEM((NB, 2, ZY, 16, CB), BF16),
        pltpu.VMEM((NB, NZ, NY, 16, CB), BF16),
        pltpu.VMEM((NB, NZ, NY, 16, CB), BF16),
        pltpu.VMEM((2, NB, 8, CB), F32),
        pltpu.VMEM((2, NB, 8, CB), F32),
        pltpu.VMEM((8, D), F32),
        pltpu.VMEM((8, D), F32),
        pltpu.VMEM((NZ, rows8, CB), F32),
        pltpu.VMEM((NX, rows8, CB), F32),
        pltpu.VMEM((NY, rows8, CB), F32),
        pltpu.VMEM((2, rows8, CB), F32),
        pltpu.VMEM((2, rows8, CB), F32),
        dma((NB2,)), dma((5,)), dma((2,)),
        dma((NB2,)), dma((NB2,)),
        dma((2, NB)), dma((2, NB)),
        dma((NB, 2)), dma((NB, 2)),
        dma((NB, 2)), dma((NB, 2)),
        dma((NB, 2)), dma((NB, 2)),
        dma((NB, NZ, NY)), dma((NB, NZ, NY)),
        dma((NB,)), dma((NB,)),
        dma((NZ,)), dma((NZ,)),
        dma((NX,)), dma((NX,)),
        dma((3, 2)), dma((3, 2)),
    ]
    any_space = pl.BlockSpec(memory_space=pl.ANY)
    vmem = pl.BlockSpec(memory_space=pltpu.VMEM)
    results = pl.pallas_call(
        functools.partial(kernel, dims),
        out_shape=[
            jax.ShapeDtypeStruct((8, D), BF16),
            jax.ShapeDtypeStruct((8, D), F32),
            jax.ShapeDtypeStruct((8, D), F32),
            jax.ShapeDtypeStruct((1, D), F32),
            jax.ShapeDtypeStruct((T, H), BF16),
        ],
        in_specs=[any_space, any_space, any_space, vmem, any_space, any_space],
        out_specs=[vmem] * 5,
        scratch_shapes=scratch,
        compiler_params=pltpu.CompilerParams(
            collective_id=0, has_side_effects=True, vmem_limit_bytes=60 * 1024 * 1024
        ),
        name="step",
    )(context, out_weight, cotangent, norm_gain.reshape(1, D), first_moment[0], second_moment[0])
    nw, n1, n2, gg, gc = delivered(results)
    return (nw[None], n1[None], n2[None], gg.reshape(D), gc)


def build(finer, block):
    sizes = tuple(finer.shape[a] for a in ("dp_0", "dp_1", "dp_2"))
    placed = (P(DP, "mp"), P("mp", None), P(DP, None), P(), P("mp", DP, None), P("mp", DP, None))
    return jax.shard_map(
        functools.partial(per_device, sizes, block),
        mesh=finer,
        in_specs=placed,
        out_specs=(P("mp", DP, None), P("mp", DP, None), P("mp", DP, None), P(), P(DP, "mp")),
        check_vma=False,
    )


def solution(mesh):
    finer = Mesh(
        mesh.devices.reshape(8, 2, 4, 2, mesh.shape["mp"]), ("dp_0", "dp_1", "dp_2", "dp_3", "mp")
    )
    return build(finer, 256)
```

```python
import functools

import jax
import jax.numpy as jnp
from jax import lax
from jax.experimental import pallas as pl
from jax.experimental.pallas import tpu as pltpu
from jax.sharding import Mesh
from jax.sharding import PartitionSpec as P

DP = ("dp_0", "dp_1", "dp_2", "dp_3")
MESH = pl.DeviceIdType.MESH
F32 = jnp.float32
BF16 = jnp.bfloat16

norm_floor = 0.1
learn_rate = 0.01
beta_one = 0.9
beta_two = 0.95
adam_floor = 1e-08

QR = 256


Z_LAGS = (1, 2, 4, 6, 8, 10)


def z_blocks(n):
    return (0, 2) if n > 2 else (0,)


def dot_nn(a, b):
    return lax.dot_general(a, b, (((1,), (0,)), ((), ())), preferred_element_type=F32)


def dot_tn(a, b):
    return lax.dot_general(a, b, (((0,), (0,)), ((), ())), preferred_element_type=F32)


def dot_nt(a, b):
    return lax.dot_general(a, b, (((1,), (1,)), ((), ())), preferred_element_type=F32)


def send(src, dst, send_sem, recv_sem, axis, peer):
    return pltpu.make_async_remote_copy(
        src_ref=src,
        dst_ref=dst,
        send_sem=send_sem,
        recv_sem=recv_sem,
        device_id={axis: peer},
        device_id_type=MESH,
    )


def landed(ref, sem):
    pltpu.make_async_copy(ref, ref, sem).wait()


def kernel(
    dims,
    ctx_hbm, w_hbm, cot_hbm, gain_ref, m1_hbm, m2_hbm,
    nw_hbm, n1_hbm, n2_hbm, gg_hbm, gc_hbm,
    nw_ref, n1_ref, n2_ref, gg_ref, gcv,
    ctx_o, ctx_s, wv, cot, att, psend, precv, ssr, spr, gaf, gas,
    grad, rx, rz, zs, zr, xs, xr, fs, gr, m1v, m2v, gz, gx, gy, gm, gk,
    ld_w, ld, c_sem, p_s, p_r, ga_s, ga_r, sa_s, sa_r, x_s, x_r, zz_s, zz_r,
    z_s, z_r, xo_s, xo_r, o_sem, f_s, f_r, gt_s, gt_r,
):
    NZ, NY, NX, TH, H, D, NB, CB = dims
    ZB = z_blocks(NB)
    NG = NZ * NY * NX
    NB2 = 2 * NB
    ZY = NZ * NY
    T = 2 * TH
    z = lax.axis_index("dp_0")
    yl = lax.axis_index("dp_1")
    x = lax.axis_index("dp_2")
    c = lax.axis_index("dp_3")
    m = lax.axis_index("mp")

    def away(me, d, n):
        return lax.rem(me + d, n)

    om, oc = 1 - m, 1 - c
    owners = [(d, e) for d in range(NZ) for e in range(NY) if (d, e) != (0, 0)]
    x_owners = [(d, e) for d in range(NX) for e in range(NY) if (d, e) != (0, 0)]

    def each_block(n, body):
        def step(i, carry):
            body(i)
            return carry

        lax.fori_loop(0, n, step, 0)

    ctx_loads = [
        pltpu.make_async_copy(ctx_hbm.at[pl.ds(k * TH, TH), :], ctx_o.at[k], ld.at[k]) for k in range(2)
    ]
    cot_load = pltpu.make_async_copy(
        cot_hbm.at[pl.ds(pl.multiple_of(m * TH, TH), TH), :], cot, ld.at[2]
    )
    m1_load = pltpu.make_async_copy(m1_hbm, m1v, ld.at[3])
    m2_load = pltpu.make_async_copy(m2_hbm, m2v, ld.at[4])

    def w_load(b):
        return pltpu.make_async_copy(
            w_hbm.at[:, pl.ds(pl.multiple_of(b * CB, CB), CB)], wv.at[b], ld_w.at[b]
        )

    for copy in ctx_loads:
        copy.start()
    each_block(NB2, lambda b: w_load(b).start())
    cot_load.start()
    m1_load.start()
    m2_load.start()

    barrier = pltpu.get_barrier_semaphore()
    peers = [{"dp_3": oc}, {"mp": om}]
    peers += [{"dp_2": away(x, d, NX), "dp_1": away(yl, e, NY)} for d, e in x_owners if d]
    peers += [{"dp_0": away(z, d, NZ), "dp_1": away(yl, e, NY)} for d, e in owners]
    for peer in peers:
        pl.semaphore_signal(barrier, inc=1, device_id=peer, device_id_type=MESH)
    with jax.named_scope("greet"):
        pl.semaphore_wait(barrier, len(peers))

    with jax.named_scope("ctx_wait"):
        for copy in ctx_loads:
            copy.wait()

    def ctx_swap():
        return send(ctx_o, ctx_s, c_sem.at[0], c_sem.at[1], "dp_3", oc)

    ctx_swap().start()

    def partial_send(b):
        return send(psend.at[b], precv.at[b], p_s.at[0], p_r.at[b], "mp", om)

    def project_theirs(b):
        w_load(b).wait()
        psend[b] = dot_nn(ctx_o[om], wv[b]).astype(BF16)
        partial_send(b).start()

    with jax.named_scope("project_theirs"):
        each_block(NB2, project_theirs)

    cot_load.wait()
    ssr[...] = jnp.zeros_like(ssr)
    spr[...] = jnp.zeros_like(spr)
    gz[z] = jnp.zeros(gz.shape[1:], F32)

    def columns(b):
        return pl.ds(pl.multiple_of(b * CB, CB), CB)

    def project_ours(b):
        att[b] = dot_nn(ctx_o[m], wv[b])

    with jax.named_scope("project_ours"):
        each_block(NB2, project_ours)

    def add_theirs(b):
        with jax.named_scope("wait_partial"):
            partial_send(b).wait_recv()
        a = att[b] + precv[b].astype(F32)
        att[b] = a
        s = cot[:, columns(b)].astype(F32) * gain_ref[:, columns(b)]
        sq, pr = a * a, a * s
        for k in range(CB // 128):
            ssr[...] += sq[:, k * 128 : (k + 1) * 128]
            spr[...] += pr[:, k * 128 : (k + 1) * 128]

    with jax.named_scope("add_theirs"):
        each_block(NB2, add_theirs)

    inverse = lax.rsqrt(jnp.sum(ssr[...], axis=1, keepdims=True) / D + norm_floor)
    mean_sn = inverse * (jnp.sum(spr[...], axis=1, keepdims=True) / D)

    def ga_send(h, j):
        return send(gaf.at[h, j, m], gaf.at[h, j, m], ga_s.at[0], ga_r.at[j], "mp", om)

    def side_send(j, who):
        return send(gaf.at[oc, j, who], gas.at[j, who], sa_s.at[0], sa_r.at[j], "dp_3", oc)

    def norm_gradient(j):
        for h in range(2):
            b = h * NB + j
            a = att[b]
            u = cot[:, columns(b)].astype(F32)
            s = u * gain_ref[:, columns(b)]
            normed = a * inverse
            gaf[h, j, m] = (inverse * (s - normed * mean_sn)).astype(BF16)
            ga_send(h, j).start()
            gz[z, pl.ds(b, 1), :] = jnp.sum(u * normed, axis=0, keepdims=True)
        side_send(j, m).start()

    with jax.named_scope("norm_gradient"):
        each_block(NB, norm_gradient)

    def gain_hop(buf, axis, me, n, ss, rs):
        return [
            send(buf.at[me], buf.at[me], ss, rs, axis, away(me, d, n)) for d in range(1, n)
        ]

    def gain_wait(buf, axis, me, n, ss, rs):
        if n > 1:
            landed(buf.at[pl.ds(0, n - 1)], rs)

    hops = [
        (gz, "dp_0", z, NZ, gt_s.at[0], gt_r.at[0]),
        (gx, "dp_2", x, NX, gt_s.at[1], gt_r.at[1]),
        (gy, "dp_1", yl, NY, gt_s.at[2], gt_r.at[2]),
        (gm, "mp", m, 2, gt_s.at[3], gt_r.at[3]),
        (gk, "dp_3", c, 2, gt_s.at[4], gt_r.at[4]),
    ]

    def summed(buf, n):
        total = buf[0]
        for i in range(1, n):
            total = total + buf[i]
        return total

    for copy in gain_hop(*hops[0]):
        copy.start()

    def gain_stage(k):
        buf, _, _, n, _, _ = hops[k]
        gain_wait(*hops[k])
        total = summed(buf, n)
        if k + 1 < len(hops):
            nxt = hops[k + 1]
            nxt[0][nxt[2]] = total
            for copy in gain_hop(*nxt):
                copy.start()
        else:
            for b in range(NB2):
                gg_ref[:, b * CB : (b + 1) * CB] = total[b : b + 1, :]

    ctx_swap().wait_recv()

    def gather_grad_attn(j):
        landed(gaf.at[:, j, om], ga_r.at[j])
        side_send(j, om).start()

    def ring(j, buf, slot, n, me, axis, ss, rs):
        size, steps = NG // n, n // 2
        half = size // 2

        def rows(t, k):
            far = steps + 1 - t
            target = away(me, far if k == 0 else n - far, n)
            if t == 1:
                return pl.ds(target * size + k * half, half)
            return pl.ds(target * size, size)

        def hop(t, k):
            peer = away(me, 1 if k == 0 else n - 1, n)
            dst = buf.at[slot, t - 1, k, pl.ds(0, half)] if t == 1 else buf.at[slot, t - 1, k]
            return send(
                grad.at[j, rows(t, k)], dst, ss.at[slot], rs.at[slot, t - 1], axis, peer
            )

        def arrived(t, k):
            return (buf[slot, t - 1, k, :half] if t == 1 else buf[slot, t - 1, k]).astype(F32)

        def wait(t):
            landed(buf.at[slot, 0, :, pl.ds(0, half)] if t == 1 else buf.at[slot, t - 1], rs.at[slot, t - 1])

        def start(t):
            for k in range(2):
                hop(t, k).start()

        def add_and_start(t):
            wait(t - 1)
            for k in range(2):
                far = steps + 1 - t
                target = away(me, far if k == 0 else n - far, n)
                if t == 2:
                    part = pl.ds(target * size + k * half, half)
                else:
                    part = pl.ds(target * size, size)
                grad[j, part] = (grad[j, part].astype(F32) + arrived(t - 1, k)).astype(BF16)
            start(t)

        def total():
            wait(steps)
            return grad[j, pl.ds(me * size, size)].astype(F32) + arrived(steps, 0) + arrived(steps, 1)

        def sent():
            landed(grad.at[j, pl.ds(0, (2 * steps - 1) * size)], ss.at[slot])

        return start, add_and_start, total, sent

    def x_ring(j):
        return ring(j, rx, j, NX, x, "dp_2", x_s, x_r)

    def z_ring(i):
        return ring(ZB[i], rz, i, NZ, z, "dp_0", zz_s, zz_r)

    def z_send(j, d, e):
        zp, yp = away(z, d, NZ), away(yl, e, NY)
        return pltpu.make_async_remote_copy(
            src_ref=zs.at[j, zp, yp],
            dst_ref=zr.at[j, d * NY + e],
            send_sem=z_s.at[j],
            recv_sem=z_r.at[j],
            device_id={"dp_0": zp, "dp_1": yp},
            device_id_type=MESH,
        )

    def core_send(j):
        return send(fs.at[oc, j], gr.at[c, j], f_s.at[0], f_r.at[0], "dp_3", oc)

    def weight_grad(j, z_first):
        landed(gas.at[j], sa_r.at[j])
        ours = gaf[c, j].reshape(T, CB)
        theirs = gas[j].reshape(T, CB)
        per = QR // 16
        for q in range(H // QR):
            cols = slice(q * QR, (q + 1) * QR)
            part = dot_tn(ctx_o[:, :, cols].reshape(T, QR), ours)
            part = part + dot_tn(ctx_s[:, :, cols].reshape(T, QR), theirs)
            part = part.astype(BF16)
            if z_first:
                grad[j, q * per : (q + 1) * per] = part.reshape(per, 16, CB)
            else:
                part = part.reshape(per // NX, NX, 16, CB)
                for k in range(NX):
                    at = k * ZY + q * (per // NX)
                    grad[j, at : at + per // NX] = part[:, k]

    def x_start(j):
        weight_grad(j, False)
        x_ring(j)[0](1)

    def x_first(j):
        x_ring(j)[1](2)

    def x_second(j):
        zs[j] = x_ring(j)[2]().astype(BF16).reshape(NZ, NY, 16, CB)
        for d, e in owners:
            z_send(j, d, e).start()

    def z_start(i):
        weight_grad(ZB[i], True)
        z_ring(i)[0](1)

    def z_last(i):
        xs[i] = z_ring(i)[2]().astype(BF16).reshape(NY, NX, 16, CB)
        for d, e in x_owners:
            xo_send(i, d, e).start()

    def x_sum(i):
        landed(xr.at[i, pl.ds(1, NX * NY - 1)], xo_r.at[i])
        total = xs[i, yl, x].astype(F32)
        for d, e in x_owners:
            total = total + xr[i, d * NY + e].astype(F32)
        to_core(ZB[i], total)

    def to_core(j, total):
        fs[0, j] = total[:8]
        fs[1, j] = total[8:]
        core_send(j).start()

    def xo_send(i, d, e):
        xp, yp = away(x, d, NX), away(yl, e, NY)
        return pltpu.make_async_remote_copy(
            src_ref=xs.at[i, yp, xp],
            dst_ref=xr.at[i, d * NY + e],
            send_sem=xo_s.at[i],
            recv_sem=xo_r.at[i],
            device_id={"dp_2": xp, "dp_1": yp},
            device_id_type=MESH,
        )

    def z_sum(j):
        landed(zr.at[j, pl.ds(1, ZY - 1)], z_r.at[j])
        total = zs[j, z, yl].astype(F32)
        for d, e in owners:
            total = total + zr[j, d * NY + e].astype(F32)
        to_core(j, total)

    def context_out(k):
        rows = pl.ds(pl.multiple_of(k * QR, QR), QR)
        return pltpu.make_async_copy(gcv.at[k], gc_hbm.at[:, rows], o_sem.at[4])

    def context_grad(k):
        rows = pl.ds(pl.multiple_of(k * QR, QR), QR)
        total = None
        for h in range(2):
            for j in range(NB):
                term = dot_nt(gaf[h, j].reshape(T, CB), wv[h * NB + j, rows, :])
                total = term if total is None else total + term
        gcv[k] = total.astype(BF16)
        context_out(k).start()

    steps_z = NZ // 2
    stages = [(x_start, 1), (x_first, 2), (x_second, 4), (z_sum, 6)]
    z_stages = [(z_start, Z_LAGS[0])]
    for n in range(2, steps_z + 1):
        z_stages.append((lambda i, n=n: z_ring(i)[1](n), Z_LAGS[n - 1]))
    z_stages += [(z_last, Z_LAGS[steps_z]), (x_sum, Z_LAGS[steps_z + 1])]
    gain_steps = (2, 4, NB + 1, NB + 2, NB + 3)
    last = max(NB + 6, max(ZB) + Z_LAGS[steps_z + 1] + 1)

    def step(t):
        for stage, lag in stages:
            mine = (t >= lag) & (t < NB + lag)
            for b in ZB:
                mine = mine & (t != b + lag)

            @pl.when(mine)
            def _():
                with jax.named_scope(stage.__name__):
                    stage(t - lag)

        for stage, lag in z_stages:
            for i, b in enumerate(ZB):

                @pl.when(t == b + lag)
                def _():
                    with jax.named_scope(f"z{lag}"):
                        stage(i)

        @pl.when(t < NB)
        def _():
            with jax.named_scope("gather"):
                gather_grad_attn(t)

        for k, when in enumerate(gain_steps):

            @pl.when(t == when)
            def _():
                with jax.named_scope("gain_stage"):
                    gain_stage(k)

        @pl.when((t >= NB) & (t < NB + H // QR))
        def _():
            with jax.named_scope("context_grad"):
                context_grad(t - NB)

    each_block(last, step)

    gr[c] = fs[c]
    m1_load.wait()
    m2_load.wait()
    with jax.named_scope("core_wait"):
        landed(gr.at[oc], f_r.at[0])
    row = pl.multiple_of(((z * NY + yl) * NX + x) * 16, 16)
    for b in range(NB2):
        cols = slice(b * CB, (b + 1) * CB)
        g = gr[b // NB, b % NB]
        first = beta_one * m1v[:, cols] + (1.0 - beta_one) * g
        second = beta_two * m2v[:, cols] + (1.0 - beta_two) * g * g
        both = wv[b, pl.ds(row, 16), :].astype(F32)
        master = jnp.where(c == 0, both[:8], both[8:])
        n1_ref[:, cols] = first
        n2_ref[:, cols] = second
        nw_ref[:, cols] = (master - learn_rate * first / (jnp.sqrt(second) + adam_floor)).astype(BF16)

    outs = [
        pltpu.make_async_copy(a, b, o_sem.at[i])
        for i, (a, b) in enumerate([(nw_ref, nw_hbm), (n1_ref, n1_hbm), (n2_ref, n2_hbm), (gg_ref, gg_hbm)])
    ]
    for copy in outs:
        copy.start()

    ctx_swap().wait_send()
    landed(psend, p_s.at[0])
    for hop in hops:
        if hop[3] > 1:
            landed(hop[0].at[pl.ds(0, hop[3] - 1)], hop[4])

    landed(gaf.at[:, :, m], ga_s.at[0])
    landed(gas, sa_s.at[0])
    landed(fs.at[oc], f_s.at[0])

    def drain(j):
        x_ring(j)[3]()
        landed(zr.at[j, pl.ds(1, ZY - 1)], z_s.at[j])

    for j in range(NB):
        if j not in ZB:
            drain(j)
    for i in range(len(ZB)):
        z_ring(i)[3]()
        landed(xr.at[i, pl.ds(1, NX * NY - 1)], xo_s.at[i])
    landed(gcv, o_sem.at[4])
    for copy in outs:
        copy.wait()


def deliver(*refs):
    n = (len(refs) - 1) // 3
    src, dst, held, sem = refs[:n], refs[n : 2 * n], refs[2 * n : 3 * n], refs[-1]
    into = [pltpu.make_async_copy(s, h, sem.at[i]) for i, (s, h) in enumerate(zip(src, held))]
    out = [pltpu.make_async_copy(h, d, sem.at[n + i]) for i, (h, d) in enumerate(zip(held, dst))]
    for copy in into:
        copy.start()
    for first, second in zip(into, out):
        first.wait()
        second.start()
    for copy in out:
        copy.wait()


def delivered(arrays):
    space = pl.BlockSpec(memory_space=pl.ANY)
    return pl.pallas_call(
        deliver,
        out_shape=[jax.ShapeDtypeStruct(a.shape, a.dtype) for a in arrays],
        in_specs=[space] * len(arrays),
        out_specs=[space] * len(arrays),
        scratch_shapes=[pltpu.VMEM(a.shape, a.dtype) for a in arrays]
        + [pltpu.SemaphoreType.DMA((2 * len(arrays),))],
        name="deliver",
    )(*arrays)


def per_device(sizes, block, context, out_weight, cotangent, norm_gain, first_moment, second_moment):
    NZ, NY, NX = sizes
    T, H = context.shape
    D = out_weight.shape[1]
    TH, CB = T // 2, block
    NB = D // (2 * CB)
    NB2 = 2 * NB
    ZY = NZ * NY
    NZB = len(z_blocks(NB))
    rows8 = (NB2 + 7) // 8 * 8
    dims = (NZ, NY, NX, TH, H, D, NB, CB)
    dma = pltpu.SemaphoreType.DMA
    scratch = [
        pltpu.VMEM((8, D), BF16),
        pltpu.VMEM((8, D), F32),
        pltpu.VMEM((8, D), F32),
        pltpu.VMEM((1, D), F32),
        pltpu.VMEM((H // QR, T, QR), BF16),
        pltpu.VMEM((2, TH, H), BF16),
        pltpu.VMEM((2, TH, H), BF16),
        pltpu.VMEM((NB2, H, CB), BF16),
        pltpu.VMEM((TH, D), BF16),
        pltpu.VMEM((NB2, TH, CB), F32),
        pltpu.VMEM((NB2, TH, CB), BF16),
        pltpu.VMEM((NB2, TH, CB), BF16),
        pltpu.VMEM((TH, 128), F32),
        pltpu.VMEM((TH, 128), F32),
        pltpu.VMEM((2, NB, 2, TH, CB), BF16),
        pltpu.VMEM((NB, 2, TH, CB), BF16),
        pltpu.VMEM((NB, NZ * NY * NX, 16, CB), BF16),
        pltpu.VMEM((NB, NX // 2, 2, ZY, 16, CB), BF16),
        pltpu.VMEM((NZB, NZ // 2, 2, NY * NX, 16, CB), BF16),
        pltpu.VMEM((NB, NZ, NY, 16, CB), BF16),
        pltpu.VMEM((NB, ZY, 16, CB), BF16),
        pltpu.VMEM((NZB, NY, NX, 16, CB), BF16),
        pltpu.VMEM((NZB, NX * NY, 16, CB), BF16),
        pltpu.VMEM((2, NB, 8, CB), F32),
        pltpu.VMEM((2, NB, 8, CB), F32),
        pltpu.VMEM((8, D), F32),
        pltpu.VMEM((8, D), F32),
        pltpu.VMEM((NZ, rows8, CB), F32),
        pltpu.VMEM((NX, rows8, CB), F32),
        pltpu.VMEM((NY, rows8, CB), F32),
        pltpu.VMEM((2, rows8, CB), F32),
        pltpu.VMEM((2, rows8, CB), F32),
        dma((NB2,)), dma((5,)), dma((2,)),
        dma((1,)), dma((NB2,)),
        dma((1,)), dma((NB,)),
        dma((1,)), dma((NB,)),
        dma((NB,)), dma((NB, NX // 2)),
        dma((NZB,)), dma((NZB, NZ // 2)),
        dma((NB,)), dma((NB,)),
        dma((NZB,)), dma((NZB,)),
        dma((5,)),
        dma((1,)), dma((1,)),
        dma((5,)), dma((5,)),
    ]
    any_space = pl.BlockSpec(memory_space=pl.ANY)
    vmem = pl.BlockSpec(memory_space=pltpu.VMEM)
    results = pl.pallas_call(
        functools.partial(kernel, dims),
        out_shape=[
            jax.ShapeDtypeStruct((8, D), BF16),
            jax.ShapeDtypeStruct((8, D), F32),
            jax.ShapeDtypeStruct((8, D), F32),
            jax.ShapeDtypeStruct((1, D), F32),
            jax.ShapeDtypeStruct((T, H), BF16),
        ],
        in_specs=[any_space, any_space, any_space, vmem, any_space, any_space],
        out_specs=[any_space] * 5,
        scratch_shapes=scratch,
        compiler_params=pltpu.CompilerParams(
            collective_id=0, has_side_effects=True, vmem_limit_bytes=60 * 1024 * 1024
        ),
        name="step",
    )(context, out_weight, cotangent, norm_gain.reshape(1, D), first_moment[0], second_moment[0])
    nw, n1, n2, gg, gc = delivered(results)
    return (nw[None], n1[None], n2[None], gg.reshape(D), gc)


def build(finer, block):
    sizes = tuple(finer.shape[a] for a in ("dp_0", "dp_1", "dp_2"))
    placed = (P(DP, "mp"), P("mp", None), P(DP, None), P(), P("mp", DP, None), P("mp", DP, None))
    return jax.shard_map(
        functools.partial(per_device, sizes, block),
        mesh=finer,
        in_specs=placed,
        out_specs=(P("mp", DP, None), P("mp", DP, None), P("mp", DP, None), P(), P(DP, "mp")),
        check_vma=False,
    )


def solution(mesh):
    finer = Mesh(
        mesh.devices.reshape(8, 2, 4, 2, mesh.shape["mp"]), ("dp_0", "dp_1", "dp_2", "dp_3", "mp")
    )
    return build(finer, 256)
```

```python
import functools

import jax
import jax.numpy as jnp
from jax import lax
from jax.experimental import pallas as pl
from jax.experimental.pallas import tpu as pltpu
from jax.sharding import Mesh
from jax.sharding import PartitionSpec as P

DP = ("dp_0", "dp_1", "dp_2", "dp_3")
MESH = pl.DeviceIdType.MESH
F32 = jnp.float32
BF16 = jnp.bfloat16

norm_floor = 0.1
learn_rate = 0.01
beta_one = 0.9
beta_two = 0.95
adam_floor = 1e-08

QR = 256


Z_PLAN = {0: (1, 2, 4, 6, 8, 10), 1: (1, 2, 4, 6, 8, 9), 3: (1, 2, 4, 5, 7, 9)}


AHEAD = 2


def z_blocks(n):
    return [b for b in Z_PLAN if b < n - 1]


def far_first(n):
    return sorted(range(n), key=lambda d: -min(d, n - d))


def dot_nn(a, b):
    return lax.dot_general(a, b, (((1,), (0,)), ((), ())), preferred_element_type=F32)


def dot_tn(a, b):
    return lax.dot_general(a, b, (((0,), (0,)), ((), ())), preferred_element_type=F32)


def dot_nt(a, b):
    return lax.dot_general(a, b, (((1,), (1,)), ((), ())), preferred_element_type=F32)


def send(src, dst, send_sem, recv_sem, axis, peer):
    return pltpu.make_async_remote_copy(
        src_ref=src,
        dst_ref=dst,
        send_sem=send_sem,
        recv_sem=recv_sem,
        device_id={axis: peer},
        device_id_type=MESH,
    )


def landed(ref, sem):
    pltpu.make_async_copy(ref, ref, sem).wait()


def kernel(
    dims,
    ctx_hbm, w_hbm, cot_hbm, gain_ref, m1_hbm, m2_hbm,
    nw_hbm, n1_hbm, n2_hbm, gg_hbm, gc_hbm,
    nw_ref, n1_ref, n2_ref, gg_ref, gcv,
    ctx_o, ctx_s, wv, cot, att, psend, precv, ssr, spr, gaf, gas,
    grad, own, ox, oz, rx, rz, zs, zr, xs, xr, fs, gr, m1v, m2v, gz, gx, gy, gm, gk,
    ld_w, ld, c_sem, p_s, p_r, ga_s, ga_r, sa_s, sa_r, x_s, x_r, zz_s, zz_r,
    z_s, z_r, xo_s, xo_r, o_sem, f_s, f_r, gt_s, gt_r,
):
    NZ, NY, NX, TH, H, D, NB, CB = dims
    ZB = z_blocks(NB)
    NG = NZ * NY * NX
    TA = TH * 4 // 5 // 16 * 16
    NB2 = 2 * NB
    ZY = NZ * NY
    T = 2 * TH
    z = lax.axis_index("dp_0")
    yl = lax.axis_index("dp_1")
    x = lax.axis_index("dp_2")
    c = lax.axis_index("dp_3")
    m = lax.axis_index("mp")

    def away(me, d, n):
        return lax.rem(me + d, n)

    om, oc = 1 - m, 1 - c
    owners = [(d, e) for d in far_first(NZ) for e in far_first(NY) if (d, e) != (0, 0)]
    x_owners = [(d, e) for d in far_first(NX) for e in far_first(NY) if (d, e) != (0, 0)]

    def each_block(n, body):
        def step(i, carry):
            body(i)
            return carry

        lax.fori_loop(0, n, step, 0)

    ctx_loads = [
        pltpu.make_async_copy(ctx_hbm.at[pl.ds(k * TH, TH), :], ctx_o.at[k], ld.at[k]) for k in range(2)
    ]
    cot_load = pltpu.make_async_copy(
        cot_hbm.at[pl.ds(pl.multiple_of(m * TH, TH), TH), :], cot, ld.at[2]
    )
    m1_load = pltpu.make_async_copy(m1_hbm, m1v, ld.at[3])
    m2_load = pltpu.make_async_copy(m2_hbm, m2v, ld.at[4])

    def w_load(b):
        return pltpu.make_async_copy(
            w_hbm.at[:, pl.ds(pl.multiple_of(b * CB, CB), CB)], wv.at[b], ld_w.at[b]
        )

    for copy in ctx_loads:
        copy.start()
    each_block(NB2, lambda b: w_load(b).start())
    cot_load.start()
    m1_load.start()
    m2_load.start()

    barrier = pltpu.get_barrier_semaphore()
    peers = [{"dp_3": oc}, {"mp": om}]
    peers += [{"dp_2": away(x, d, NX), "dp_1": away(yl, e, NY)} for d, e in x_owners if d]
    peers += [{"dp_0": away(z, d, NZ), "dp_1": away(yl, e, NY)} for d, e in owners]
    for peer in peers:
        pl.semaphore_signal(barrier, inc=1, device_id=peer, device_id_type=MESH)
    with jax.named_scope("greet"):
        pl.semaphore_wait(barrier, len(peers))

    with jax.named_scope("ctx_wait"):
        for copy in ctx_loads:
            copy.wait()

    def ctx_swap():
        return send(ctx_o, ctx_s, c_sem.at[0], c_sem.at[1], "dp_3", oc)

    ctx_swap().start()

    head, tail = slice(0, TA), slice(TA, TH)

    def partial_send(b):
        return send(psend.at[b, head], precv.at[b, head], p_s.at[0], p_r.at[b], "mp", om)

    def partial_rest():
        return send(psend.at[:, tail], precv.at[:, tail], p_s.at[0], p_r.at[NB2], "mp", om)

    def project_theirs(b):
        w_load(b).wait()
        psend[b] = dot_nn(ctx_o[om], wv[b]).astype(BF16)
        partial_send(b).start()

    with jax.named_scope("project_theirs"):
        each_block(NB2, project_theirs)

    partial_rest().start()
    cot_load.wait()
    ssr[...] = jnp.zeros_like(ssr)
    spr[...] = jnp.zeros_like(spr)
    gz[z] = jnp.zeros(gz.shape[1:], F32)

    def columns(b):
        return pl.ds(pl.multiple_of(b * CB, CB), CB)

    def project_ours(b):
        att[b] = dot_nn(ctx_o[m], wv[b])

    with jax.named_scope("project_ours"):
        each_block(NB2, project_ours)

    def add_theirs(b, rows):
        a = att[b, rows] + precv[b, rows].astype(F32)
        att[b, rows] = a
        s = cot[rows, columns(b)].astype(F32) * gain_ref[columns(b)][None, :]
        sq, pr = a * a, a * s
        for k in range(CB // 128):
            ssr[rows] += sq[:, k * 128 : (k + 1) * 128]
            spr[rows] += pr[:, k * 128 : (k + 1) * 128]

    def add_head(b):
        with jax.named_scope("wait_partial"):
            partial_send(b).wait_recv()
        add_theirs(b, head)

    with jax.named_scope("add_head"):
        each_block(NB2, add_head)

    def row_terms(rows):
        inverse = lax.rsqrt(jnp.sum(ssr[rows], axis=1, keepdims=True) / D + norm_floor)
        return inverse, inverse * (jnp.sum(spr[rows], axis=1, keepdims=True) / D)

    def ga_send(j, rows):
        part = gaf.at[:, j, m, rows]
        return send(part, part, ga_s.at[0], ga_r.at[j], "mp", om)

    def side_send(j, who):
        return send(gaf.at[oc, j, who], gas.at[j, who], sa_s.at[0], sa_r.at[j], "dp_3", oc)

    def norm_gradient(j, rows, terms):
        inverse, mean_sn = terms
        for h in range(2):
            b = h * NB + j
            u = cot[rows, columns(b)].astype(F32)
            s = u * gain_ref[columns(b)][None, :]
            normed = att[b, rows] * inverse
            gaf[h, j, m, rows] = (inverse * (s - normed * mean_sn)).astype(BF16)
            gz[z, pl.ds(b, 1), :] += jnp.sum(u * normed, axis=0, keepdims=True)
        ga_send(j, rows).start()

    head_terms = row_terms(head)
    with jax.named_scope("norm_head"):
        each_block(AHEAD, lambda j: norm_gradient(j, head, head_terms))
    with jax.named_scope("add_tail"):
        partial_rest().wait_recv()
        each_block(NB2, lambda b: add_theirs(b, tail))
    tail_terms = row_terms(tail)

    def norm_tail(j):
        norm_gradient(j, tail, tail_terms)
        side_send(j, m).start()

    def norm_both(j):
        norm_gradient(j, head, head_terms)
        norm_tail(j)

    with jax.named_scope("norm_tail"):
        each_block(AHEAD, norm_tail)
        each_block(NB - AHEAD, lambda j: norm_both(j + AHEAD))

    def gain_hop(buf, axis, me, n, ss, rs):
        return [
            send(buf.at[me], buf.at[me], ss, rs, axis, away(me, d, n)) for d in range(1, n)
        ]

    def gain_wait(buf, axis, me, n, ss, rs):
        if n > 1:
            landed(buf.at[pl.ds(0, n - 1)], rs)

    hops = [
        (gz, "dp_0", z, NZ, gt_s.at[0], gt_r.at[0]),
        (gx, "dp_2", x, NX, gt_s.at[1], gt_r.at[1]),
        (gy, "dp_1", yl, NY, gt_s.at[2], gt_r.at[2]),
        (gm, "mp", m, 2, gt_s.at[3], gt_r.at[3]),
        (gk, "dp_3", c, 2, gt_s.at[4], gt_r.at[4]),
    ]

    def summed(buf, n):
        total = buf[0]
        for i in range(1, n):
            total = total + buf[i]
        return total

    for copy in gain_hop(*hops[0]):
        copy.start()

    def gain_stage(k):
        buf, _, _, n, _, _ = hops[k]
        gain_wait(*hops[k])
        total = summed(buf, n)
        if k + 1 < len(hops):
            nxt = hops[k + 1]
            nxt[0][nxt[2]] = total
            for copy in gain_hop(*nxt):
                copy.start()
        else:
            for b in range(NB2):
                gg_ref[b * CB : (b + 1) * CB] = total[b]

    ctx_swap().wait_recv()

    def gather_grad_attn(j):
        landed(gaf.at[:, j, om], ga_r.at[j])
        side_send(j, om).start()

    def ring(j, out, buf, slot, n, me, axis, ss, rs):
        size, steps = NG // n, n // 2
        half = size // 2

        def target(t, k):
            far = steps + 1 - t
            return away(me, far if k == 0 else n - far, n) * size

        def out_rows(t, k):
            if t == 1:
                return pl.ds(k * half, half)
            return pl.ds(size + (t - 2) * 2 * size + k * size, size)

        def hop(t, k):
            peer = away(me, 1 if k == 0 else n - 1, n)
            dst = buf.at[slot, t - 1, k, pl.ds(0, half)] if t == 1 else buf.at[slot, t - 1, k]
            return send(out.at[slot, out_rows(t, k)], dst, ss.at[slot], rs.at[slot, t - 1], axis, peer)

        def arrived(t, k):
            return (buf[slot, t - 1, k, :half] if t == 1 else buf[slot, t - 1, k]).astype(F32)

        def wait(t):
            landed(buf.at[slot, 0, :, pl.ds(0, half)] if t == 1 else buf.at[slot, t - 1], rs.at[slot, t - 1])

        def start():
            for k in range(2):
                out[slot, out_rows(1, k)] = grad[j, pl.ds(target(1, k) + k * half, half)].astype(BF16)
            for k in range(2):
                hop(1, k).start()

        def add_and_start(t):
            wait(t - 1)
            for k in range(2):
                at = target(t, k)
                if t == 2:
                    base = size + k * size
                    mine, other = k * half, (1 - k) * half
                    total = grad[j, pl.ds(at + mine, half)] + arrived(1, k)
                    out[slot, base + mine : base + mine + half] = total.astype(BF16)
                    rest = grad[j, pl.ds(at + other, half)]
                    out[slot, base + other : base + other + half] = rest.astype(BF16)
                else:
                    total = grad[j, pl.ds(at, size)] + arrived(t - 1, k)
                    out[slot, out_rows(t, k)] = total.astype(BF16)
            for k in range(2):
                hop(t, k).start()

        def total():
            wait(steps)
            return grad[j, pl.ds(me * size, size)] + arrived(steps, 0) + arrived(steps, 1)

        def sent():
            landed(out.at[slot], ss.at[slot])

        return start, add_and_start, total, sent

    def x_ring(j):
        return ring(j, ox, rx, j, NX, x, "dp_2", x_s, x_r)

    def z_ring(i):
        return ring(ZB[i], oz, rz, i, NZ, z, "dp_0", zz_s, zz_r)

    def z_send(j, d, e):
        zp, yp = away(z, d, NZ), away(yl, e, NY)
        return pltpu.make_async_remote_copy(
            src_ref=zs.at[j, zp, yp],
            dst_ref=zr.at[j, d * NY + e],
            send_sem=z_s.at[j],
            recv_sem=z_r.at[j],
            device_id={"dp_0": zp, "dp_1": yp},
            device_id_type=MESH,
        )

    def core_send(j):
        return send(fs.at[oc, j], gr.at[c, j], f_s.at[0], f_r.at[0], "dp_3", oc)

    def weight_grad(j, z_first):
        landed(gas.at[j], sa_r.at[j])
        ours = gaf[c, j].reshape(T, CB)
        theirs = gas[j].reshape(T, CB)
        per = QR // 16
        for q in range(H // QR):
            cols = slice(q * QR, (q + 1) * QR)
            part = dot_tn(ctx_o[:, :, cols].reshape(T, QR), ours)
            part = part + dot_tn(ctx_s[:, :, cols].reshape(T, QR), theirs)
            if z_first:
                grad[j, q * per : (q + 1) * per] = part.reshape(per, 16, CB)
            else:
                part = part.reshape(per // NX, NX, 16, CB)
                for k in range(NX):
                    at = k * ZY + q * (per // NX)
                    grad[j, at : at + per // NX] = part[:, k]

    def x_start(j):
        weight_grad(j, False)
        x_ring(j)[0]()

    def x_first(j):
        x_ring(j)[1](2)

    def x_second(j):
        total = x_ring(j)[2]()
        own[j] = total
        zs[j] = total.astype(BF16).reshape(NZ, NY, 16, CB)
        for d, e in owners:
            z_send(j, d, e).start()

    def z_start(i):
        weight_grad(ZB[i], True)
        z_ring(i)[0]()

    def z_last(i):
        total = z_ring(i)[2]()
        own[ZB[i], : NY * NX] = total
        xs[i] = total.astype(BF16).reshape(NY, NX, 16, CB)
        for d, e in x_owners:
            xo_send(i, d, e).start()

    def x_sum(i):
        landed(xr.at[i, pl.ds(1, NX * NY - 1)], xo_r.at[i])
        total = own[ZB[i], yl * NX + x]
        for d, e in x_owners:
            total = total + xr[i, d * NY + e].astype(F32)
        to_core(ZB[i], total)

    def to_core(j, total):
        fs[0, j] = total[:8]
        fs[1, j] = total[8:]
        core_send(j).start()

    def xo_send(i, d, e):
        xp, yp = away(x, d, NX), away(yl, e, NY)
        return pltpu.make_async_remote_copy(
            src_ref=xs.at[i, yp, xp],
            dst_ref=xr.at[i, d * NY + e],
            send_sem=xo_s.at[i],
            recv_sem=xo_r.at[i],
            device_id={"dp_2": xp, "dp_1": yp},
            device_id_type=MESH,
        )

    def z_sum(j):
        landed(zr.at[j, pl.ds(1, ZY - 1)], z_r.at[j])
        total = own[j, z * NY + yl]
        for d, e in owners:
            total = total + zr[j, d * NY + e].astype(F32)
        to_core(j, total)

    def context_out(k):
        rows = pl.ds(pl.multiple_of(k * QR, QR), QR)
        return pltpu.make_async_copy(gcv.at[k], gc_hbm.at[:, rows], o_sem.at[4])

    def context_grad(k):
        rows = pl.ds(pl.multiple_of(k * QR, QR), QR)
        total = None
        for h in range(2):
            for j in range(NB):
                term = dot_nt(gaf[h, j].reshape(T, CB), wv[h * NB + j, rows, :])
                total = term if total is None else total + term
        gcv[k] = total.astype(BF16)
        context_out(k).start()

    steps_z = NZ // 2
    stages = [(x_start, 1), (x_first, 2), (x_second, 4), (z_sum, 6)]
    z_stages = [z_start]
    z_stages += [lambda i, n=n: z_ring(i)[1](n) for n in range(2, steps_z + 1)]
    z_stages += [z_last, x_sum]
    gain_steps = (2, 4, NB, NB + 3, NB + 5)
    last = max([NB + 6] + [b + Z_PLAN[b][steps_z + 1] + 1 for b in ZB])

    def step(t):
        for stage, lag in stages:
            mine = (t >= lag) & (t < NB + lag)
            for b in ZB:
                mine = mine & (t != b + lag)

            @pl.when(mine)
            def _():
                with jax.named_scope(stage.__name__):
                    stage(t - lag)

        for n, stage in enumerate(z_stages):
            for i, b in enumerate(ZB):

                @pl.when(t == b + Z_PLAN[b][n])
                def _():
                    with jax.named_scope(f"z{n}#b={b}"):
                        stage(i)

        @pl.when(t < NB)
        def _():
            with jax.named_scope("gather"):
                gather_grad_attn(t)

        for k, when in enumerate(gain_steps):

            @pl.when(t == when)
            def _():
                with jax.named_scope("gain_stage"):
                    gain_stage(k)

        @pl.when((t >= NB) & (t < NB + H // QR))
        def _():
            with jax.named_scope("context_grad"):
                context_grad(t - NB)

    each_block(last, step)

    gr[c] = fs[c]
    m1_load.wait()
    m2_load.wait()
    with jax.named_scope("core_wait"):
        landed(gr.at[oc], f_r.at[0])
    row = pl.multiple_of(((z * NY + yl) * NX + x) * 16, 16)
    for b in range(NB2):
        cols = slice(b * CB, (b + 1) * CB)
        g = gr[b // NB, b % NB]
        first = beta_one * m1v[:, cols] + (1.0 - beta_one) * g
        second = beta_two * m2v[:, cols] + (1.0 - beta_two) * g * g
        both = wv[b, pl.ds(row, 16), :].astype(F32)
        master = jnp.where(c == 0, both[:8], both[8:])
        n1_ref[:, cols] = first
        n2_ref[:, cols] = second
        nw_ref[:, cols] = (master - learn_rate * first / (jnp.sqrt(second) + adam_floor)).astype(BF16)

    outs = [
        pltpu.make_async_copy(a, b, o_sem.at[i])
        for i, (a, b) in enumerate([(nw_ref, nw_hbm), (n1_ref, n1_hbm), (n2_ref, n2_hbm), (gg_ref, gg_hbm)])
    ]
    for copy in outs:
        copy.start()

    ctx_swap().wait_send()
    landed(psend, p_s.at[0])
    for hop in hops:
        if hop[3] > 1:
            landed(hop[0].at[pl.ds(0, hop[3] - 1)], hop[4])

    landed(gaf.at[:, :, m], ga_s.at[0])
    landed(gas, sa_s.at[0])
    landed(fs.at[oc], f_s.at[0])

    def drain(j):
        x_ring(j)[3]()
        landed(zr.at[j, pl.ds(1, ZY - 1)], z_s.at[j])

    for j in range(NB):
        if j not in ZB:
            drain(j)
    for i in range(len(ZB)):
        z_ring(i)[3]()
        landed(xr.at[i, pl.ds(1, NX * NY - 1)], xo_s.at[i])
    landed(gcv, o_sem.at[4])
    for copy in outs:
        copy.wait()


def deliver(*refs):
    n = (len(refs) - 1) // 3
    src, dst, held, sem = refs[:n], refs[n : 2 * n], refs[2 * n : 3 * n], refs[-1]
    into = [pltpu.make_async_copy(s, h, sem.at[i]) for i, (s, h) in enumerate(zip(src, held))]
    out = [pltpu.make_async_copy(h, d, sem.at[n + i]) for i, (h, d) in enumerate(zip(held, dst))]
    for copy in into:
        copy.start()
    for first, second in zip(into, out):
        first.wait()
        second.start()
    for copy in out:
        copy.wait()


def delivered(arrays):
    space = pl.BlockSpec(memory_space=pl.ANY)
    return pl.pallas_call(
        deliver,
        out_shape=[jax.ShapeDtypeStruct(a.shape, a.dtype) for a in arrays],
        in_specs=[space] * len(arrays),
        out_specs=[space] * len(arrays),
        scratch_shapes=[pltpu.VMEM(a.shape, a.dtype) for a in arrays]
        + [pltpu.SemaphoreType.DMA((2 * len(arrays),))],
        name="deliver",
    )(*arrays)


def per_device(sizes, block, context, out_weight, cotangent, norm_gain, first_moment, second_moment):
    NZ, NY, NX = sizes
    T, H = context.shape
    D = out_weight.shape[1]
    TH, CB = T // 2, block
    NB = D // (2 * CB)
    NB2 = 2 * NB
    ZY = NZ * NY
    NZB = len(z_blocks(NB))
    rows8 = (NB2 + 7) // 8 * 8
    dims = (NZ, NY, NX, TH, H, D, NB, CB)
    dma = pltpu.SemaphoreType.DMA
    scratch = [
        pltpu.VMEM((8, D), BF16),
        pltpu.VMEM((8, D), F32),
        pltpu.VMEM((8, D), F32),
        pltpu.VMEM((D,), F32),
        pltpu.VMEM((H // QR, T, QR), BF16),
        pltpu.VMEM((2, TH, H), BF16),
        pltpu.VMEM((2, TH, H), BF16),
        pltpu.VMEM((NB2, H, CB), BF16),
        pltpu.VMEM((TH, D), BF16),
        pltpu.VMEM((NB2, TH, CB), F32),
        pltpu.VMEM((NB2, TH, CB), BF16),
        pltpu.VMEM((NB2, TH, CB), BF16),
        pltpu.VMEM((TH, 128), F32),
        pltpu.VMEM((TH, 128), F32),
        pltpu.VMEM((2, NB, 2, TH, CB), BF16),
        pltpu.VMEM((NB, 2, TH, CB), BF16),
        pltpu.VMEM((NB, NZ * NY * NX, 16, CB), F32),
        pltpu.VMEM((NB, max(ZY, NY * NX), 16, CB), F32),
        pltpu.VMEM((NB, (NX - 1) * ZY, 16, CB), BF16),
        pltpu.VMEM((NZB, (NZ - 1) * NY * NX, 16, CB), BF16),
        pltpu.VMEM((NB, NX // 2, 2, ZY, 16, CB), BF16),
        pltpu.VMEM((NZB, NZ // 2, 2, NY * NX, 16, CB), BF16),
        pltpu.VMEM((NB, NZ, NY, 16, CB), BF16),
        pltpu.VMEM((NB, ZY, 16, CB), BF16),
        pltpu.VMEM((NZB, NY, NX, 16, CB), BF16),
        pltpu.VMEM((NZB, NX * NY, 16, CB), BF16),
        pltpu.VMEM((2, NB, 8, CB), F32),
        pltpu.VMEM((2, NB, 8, CB), F32),
        pltpu.VMEM((8, D), F32),
        pltpu.VMEM((8, D), F32),
        pltpu.VMEM((NZ, rows8, CB), F32),
        pltpu.VMEM((NX, rows8, CB), F32),
        pltpu.VMEM((NY, rows8, CB), F32),
        pltpu.VMEM((2, rows8, CB), F32),
        pltpu.VMEM((2, rows8, CB), F32),
        dma((NB2,)), dma((5,)), dma((2,)),
        dma((1,)), dma((NB2 + 1,)),
        dma((1,)), dma((NB,)),
        dma((1,)), dma((NB,)),
        dma((NB,)), dma((NB, NX // 2)),
        dma((NZB,)), dma((NZB, NZ // 2)),
        dma((NB,)), dma((NB,)),
        dma((NZB,)), dma((NZB,)),
        dma((5,)),
        dma((1,)), dma((1,)),
        dma((5,)), dma((5,)),
    ]
    any_space = pl.BlockSpec(memory_space=pl.ANY)
    vmem = pl.BlockSpec(memory_space=pltpu.VMEM)
    results = pl.pallas_call(
        functools.partial(kernel, dims),
        out_shape=[
            jax.ShapeDtypeStruct((8, D), BF16),
            jax.ShapeDtypeStruct((8, D), F32),
            jax.ShapeDtypeStruct((8, D), F32),
            jax.ShapeDtypeStruct((D,), F32),
            jax.ShapeDtypeStruct((T, H), BF16),
        ],
        in_specs=[any_space, any_space, any_space, vmem, any_space, any_space],
        out_specs=[any_space] * 5,
        scratch_shapes=scratch,
        compiler_params=pltpu.CompilerParams(
            collective_id=0, has_side_effects=True, vmem_limit_bytes=60 * 1024 * 1024
        ),
        name="step",
    )(context, out_weight, cotangent, norm_gain, first_moment[0], second_moment[0])
    nw, n1, n2, gg, gc = delivered(results)
    return (nw[None], n1[None], n2[None], gg, gc)


def build(finer, block):
    sizes = tuple(finer.shape[a] for a in ("dp_0", "dp_1", "dp_2"))
    placed = (P(DP, "mp"), P("mp", None), P(DP, None), P(), P("mp", DP, None), P("mp", DP, None))
    return jax.shard_map(
        functools.partial(per_device, sizes, block),
        mesh=finer,
        in_specs=placed,
        out_specs=(P("mp", DP, None), P("mp", DP, None), P("mp", DP, None), P(), P(DP, "mp")),
        check_vma=False,
    )


def solution(mesh):
    finer = Mesh(
        mesh.devices.reshape(8, 2, 4, 2, mesh.shape["mp"]), ("dp_0", "dp_1", "dp_2", "dp_3", "mp")
    )
    return build(finer, 256)
```

```python
import functools

import jax
import jax.numpy as jnp
from jax import lax
from jax.experimental import pallas as pl
from jax.experimental.pallas import tpu as pltpu
from jax.sharding import Mesh
from jax.sharding import PartitionSpec as P

DP = ("dp_0", "dp_1", "dp_2", "dp_3")
MESH = pl.DeviceIdType.MESH
F32 = jnp.float32
BF16 = jnp.bfloat16

norm_floor = 0.1
learn_rate = 0.01
beta_one = 0.9
beta_two = 0.95
adam_floor = 1e-08

QR = 256


Z_PLAN = {0: (0, 1, 3, 5, 7, 9), 1: (0, 1, 3, 5, 7, 8), 3: (0, 1, 3, 4, 6, 8)}


AHEAD = 2


def z_blocks(n):
    return [b for b in Z_PLAN if b < n - 1]


def far_first(n):
    return sorted(range(n), key=lambda d: -min(d, n - d))


def dot_nn(a, b):
    return lax.dot_general(a, b, (((1,), (0,)), ((), ())), preferred_element_type=F32)


def dot_tn(a, b):
    return lax.dot_general(a, b, (((0,), (0,)), ((), ())), preferred_element_type=F32)


def dot_nt(a, b):
    return lax.dot_general(a, b, (((1,), (1,)), ((), ())), preferred_element_type=F32)


def send(src, dst, send_sem, recv_sem, axis, peer):
    return pltpu.make_async_remote_copy(
        src_ref=src,
        dst_ref=dst,
        send_sem=send_sem,
        recv_sem=recv_sem,
        device_id={axis: peer},
        device_id_type=MESH,
    )


def landed(ref, sem):
    pltpu.make_async_copy(ref, ref, sem).wait()


def kernel(
    dims,
    ctx_hbm, w_hbm, cot_hbm, gain_ref, m1_hbm, m2_hbm,
    nw_hbm, n1_hbm, n2_hbm, gg_hbm, gc_hbm,
    nw_ref, n1_ref, n2_ref, gg_ref, gcv, gcs, gcr, gcb,
    ctx_o, ctx_s, wv, cot, att, psend, precv, ssr, spr, gaf, gas,
    grad, own, ox, oz, rx, rz, zs, zr, xs, xr, fs, gr, m1v, m2v, gz, gx, gy, gm, gk,
    ld_w, ld, c_sem, p_s, p_r, ga_s, ga_r, sa_s, sa_r, x_s, x_r, zz_s, zz_r,
    z_s, z_r, xo_s, xo_r, o_sem, f_s, f_r, gt_s, gt_r, gc_s,
):
    NZ, NY, NX, TH, H, D, NB, CB = dims
    ZB = z_blocks(NB)
    NG = NZ * NY * NX
    TA = TH * 4 // 5 // 16 * 16
    NB2 = 2 * NB
    ZY = NZ * NY
    T = 2 * TH
    z = lax.axis_index("dp_0")
    yl = lax.axis_index("dp_1")
    x = lax.axis_index("dp_2")
    c = lax.axis_index("dp_3")
    m = lax.axis_index("mp")

    def away(me, d, n):
        return lax.rem(me + d, n)

    om, oc = 1 - m, 1 - c
    owners = [(d, e) for d in far_first(NZ) for e in far_first(NY) if (d, e) != (0, 0)]
    x_owners = [(d, e) for d in far_first(NX) for e in far_first(NY) if (d, e) != (0, 0)]

    def each_block(n, body):
        def step(i, carry):
            body(i)
            return carry

        lax.fori_loop(0, n, step, 0)

    ctx_loads = [
        pltpu.make_async_copy(ctx_hbm.at[pl.ds(k * TH, TH), :], ctx_o.at[k], ld.at[k]) for k in range(2)
    ]
    cot_load = pltpu.make_async_copy(
        cot_hbm.at[pl.ds(pl.multiple_of(m * TH, TH), TH), :], cot, ld.at[2]
    )
    m1_load = pltpu.make_async_copy(m1_hbm, m1v, ld.at[3])
    m2_load = pltpu.make_async_copy(m2_hbm, m2v, ld.at[4])

    def w_load(b):
        return pltpu.make_async_copy(
            w_hbm.at[:, pl.ds(pl.multiple_of(b * CB, CB), CB)], wv.at[b], ld_w.at[b]
        )

    for copy in ctx_loads:
        copy.start()
    each_block(NB2, lambda b: w_load(b).start())
    cot_load.start()
    m1_load.start()
    m2_load.start()

    barrier = pltpu.get_barrier_semaphore()
    peers = [{"dp_3": oc}, {"mp": om}, {"mp": om, "dp_3": oc}]
    peers += [{"dp_2": away(x, d, NX), "dp_1": away(yl, e, NY)} for d, e in x_owners if d]
    peers += [{"dp_0": away(z, d, NZ), "dp_1": away(yl, e, NY)} for d, e in owners]
    for peer in peers:
        pl.semaphore_signal(barrier, inc=1, device_id=peer, device_id_type=MESH)
    with jax.named_scope("greet"):
        pl.semaphore_wait(barrier, len(peers))

    with jax.named_scope("ctx_wait"):
        for copy in ctx_loads:
            copy.wait()

    def ctx_swap():
        return send(ctx_o, ctx_s, c_sem.at[0], c_sem.at[1], "dp_3", oc)

    ctx_swap().start()

    head, tail = slice(0, TA), slice(TA, TH)

    def partial_send(b):
        return send(psend.at[b, head], precv.at[b, head], p_s.at[0], p_r.at[b], "mp", om)

    def partial_rest():
        return send(psend.at[:, tail], precv.at[:, tail], p_s.at[0], p_r.at[NB2], "mp", om)

    def project_theirs(b):
        w_load(b).wait()
        psend[b] = dot_nn(ctx_o[om], wv[b]).astype(BF16)
        partial_send(b).start()

    with jax.named_scope("project_theirs"):
        each_block(NB2, project_theirs)

    partial_rest().start()
    cot_load.wait()
    ssr[...] = jnp.zeros_like(ssr)
    spr[...] = jnp.zeros_like(spr)
    gz[z] = jnp.zeros(gz.shape[1:], F32)

    def columns(b):
        return pl.ds(pl.multiple_of(b * CB, CB), CB)

    def project_ours(b):
        att[b] = dot_nn(ctx_o[m], wv[b])

    with jax.named_scope("project_ours"):
        each_block(NB2, project_ours)

    def add_theirs(b, rows):
        a = att[b, rows] + precv[b, rows].astype(F32)
        att[b, rows] = a
        s = cot[rows, columns(b)].astype(F32) * gain_ref[columns(b)][None, :]
        sq, pr = a * a, a * s
        for k in range(CB // 128):
            ssr[rows] += sq[:, k * 128 : (k + 1) * 128]
            spr[rows] += pr[:, k * 128 : (k + 1) * 128]

    def add_head(b):
        with jax.named_scope("wait_partial"):
            partial_send(b).wait_recv()
        add_theirs(b, head)

    with jax.named_scope("add_head"):
        each_block(NB2, add_head)

    def row_terms(rows):
        inverse = lax.rsqrt(jnp.sum(ssr[rows], axis=1, keepdims=True) / D + norm_floor)
        return inverse, inverse * (jnp.sum(spr[rows], axis=1, keepdims=True) / D)

    def ga_sends(j, rows):
        here, there = gaf.at[c, j, m, rows], gaf.at[oc, j, m, rows]
        straight = send(here, here, ga_s.at[0], ga_r.at[j], "mp", om)
        crossed = pltpu.make_async_remote_copy(
            src_ref=there,
            dst_ref=gas.at[j, m, rows],
            send_sem=ga_s.at[0],
            recv_sem=sa_r.at[j],
            device_id={"mp": om, "dp_3": oc},
            device_id_type=MESH,
        )
        return straight, crossed

    def side_send(j):
        return send(gaf.at[oc, j, m], gas.at[j, m], sa_s.at[0], sa_r.at[j], "dp_3", oc)

    def norm_gradient(j, rows, terms):
        inverse, mean_sn = terms
        for h in range(2):
            b = h * NB + j
            u = cot[rows, columns(b)].astype(F32)
            s = u * gain_ref[columns(b)][None, :]
            normed = att[b, rows] * inverse
            gaf[h, j, m, rows] = (inverse * (s - normed * mean_sn)).astype(BF16)
            gz[z, pl.ds(b, 1), :] += jnp.sum(u * normed, axis=0, keepdims=True)
        for copy in ga_sends(j, rows):
            copy.start()

    head_terms = row_terms(head)
    with jax.named_scope("norm_head"):
        each_block(AHEAD, lambda j: norm_gradient(j, head, head_terms))
    with jax.named_scope("add_tail"):
        partial_rest().wait_recv()
        each_block(NB2, lambda b: add_theirs(b, tail))
    tail_terms = row_terms(tail)

    def norm_tail(j):
        norm_gradient(j, tail, tail_terms)
        side_send(j).start()

    def norm_both(j):
        norm_gradient(j, head, head_terms)
        norm_tail(j)

    with jax.named_scope("norm_tail"):
        each_block(AHEAD, norm_tail)
        each_block(NB - AHEAD, lambda j: norm_both(j + AHEAD))

    def gain_hop(buf, axis, me, n, ss, rs):
        return [
            send(buf.at[me], buf.at[me], ss, rs, axis, away(me, d, n)) for d in range(1, n)
        ]

    def gain_wait(buf, axis, me, n, ss, rs):
        if n > 1:
            landed(buf.at[pl.ds(0, n - 1)], rs)

    hops = [
        (gz, "dp_0", z, NZ, gt_s.at[0], gt_r.at[0]),
        (gx, "dp_2", x, NX, gt_s.at[1], gt_r.at[1]),
        (gy, "dp_1", yl, NY, gt_s.at[2], gt_r.at[2]),
        (gm, "mp", m, 2, gt_s.at[3], gt_r.at[3]),
        (gk, "dp_3", c, 2, gt_s.at[4], gt_r.at[4]),
    ]

    def summed(buf, n):
        total = buf[0]
        for i in range(1, n):
            total = total + buf[i]
        return total

    for copy in gain_hop(*hops[0]):
        copy.start()

    def gain_stage(k):
        buf, _, _, n, _, _ = hops[k]
        gain_wait(*hops[k])
        total = summed(buf, n)
        if k + 1 < len(hops):
            nxt = hops[k + 1]
            nxt[0][nxt[2]] = total
            for copy in gain_hop(*nxt):
                copy.start()
        else:
            for b in range(NB2):
                gg_ref[b * CB : (b + 1) * CB] = total[b]

    ctx_swap().wait_recv()

    def ring(j, out, buf, slot, n, me, axis, ss, rs):
        size, steps = NG // n, n // 2
        half = size // 2

        def target(t, k):
            far = steps + 1 - t
            return away(me, far if k == 0 else n - far, n) * size

        def out_rows(t, k):
            if t == 1:
                return pl.ds(k * half, half)
            return pl.ds(size + (t - 2) * 2 * size + k * size, size)

        def hop(t, k):
            peer = away(me, 1 if k == 0 else n - 1, n)
            dst = buf.at[slot, t - 1, k, pl.ds(0, half)] if t == 1 else buf.at[slot, t - 1, k]
            return send(out.at[slot, out_rows(t, k)], dst, ss.at[slot], rs.at[slot, t - 1], axis, peer)

        def arrived(t, k):
            return (buf[slot, t - 1, k, :half] if t == 1 else buf[slot, t - 1, k]).astype(F32)

        def wait(t):
            landed(buf.at[slot, 0, :, pl.ds(0, half)] if t == 1 else buf.at[slot, t - 1], rs.at[slot, t - 1])

        def start():
            for k in range(2):
                out[slot, out_rows(1, k)] = grad[j, pl.ds(target(1, k) + k * half, half)].astype(BF16)
            for k in range(2):
                hop(1, k).start()

        def add_and_start(t):
            wait(t - 1)
            for k in range(2):
                at = target(t, k)
                if t == 2:
                    base = size + k * size
                    mine, other = k * half, (1 - k) * half
                    total = grad[j, pl.ds(at + mine, half)] + arrived(1, k)
                    out[slot, base + mine : base + mine + half] = total.astype(BF16)
                    rest = grad[j, pl.ds(at + other, half)]
                    out[slot, base + other : base + other + half] = rest.astype(BF16)
                else:
                    total = grad[j, pl.ds(at, size)] + arrived(t - 1, k)
                    out[slot, out_rows(t, k)] = total.astype(BF16)
            for k in range(2):
                hop(t, k).start()

        def total():
            wait(steps)
            return grad[j, pl.ds(me * size, size)] + arrived(steps, 0) + arrived(steps, 1)

        def sent():
            landed(out.at[slot], ss.at[slot])

        return start, add_and_start, total, sent

    def x_ring(j):
        return ring(j, ox, rx, j, NX, x, "dp_2", x_s, x_r)

    def z_ring(i):
        return ring(ZB[i], oz, rz, i, NZ, z, "dp_0", zz_s, zz_r)

    def z_send(j, d, e):
        zp, yp = away(z, d, NZ), away(yl, e, NY)
        return pltpu.make_async_remote_copy(
            src_ref=zs.at[j, zp, yp],
            dst_ref=zr.at[j, d * NY + e],
            send_sem=z_s.at[j],
            recv_sem=z_r.at[j],
            device_id={"dp_0": zp, "dp_1": yp},
            device_id_type=MESH,
        )

    def core_send(j):
        return send(fs.at[oc, j], gr.at[c, j], f_s.at[0], f_r.at[0], "dp_3", oc)

    def weight_grad(j, z_first):
        landed(gaf.at[c, j, om], ga_r.at[j])
        landed(gas.at[j], sa_r.at[j])
        ours = gaf[c, j].reshape(T, CB)
        theirs = gas[j].reshape(T, CB)
        per = QR // 16
        for q in range(H // QR):
            cols = slice(q * QR, (q + 1) * QR)
            part = dot_tn(ctx_o[:, :, cols].reshape(T, QR), ours)
            part = part + dot_tn(ctx_s[:, :, cols].reshape(T, QR), theirs)
            if z_first:
                grad[j, q * per : (q + 1) * per] = part.reshape(per, 16, CB)
            else:
                part = part.reshape(per // NX, NX, 16, CB)
                for k in range(NX):
                    at = k * ZY + q * (per // NX)
                    grad[j, at : at + per // NX] = part[:, k]

    def x_start(j):
        weight_grad(j, False)
        x_ring(j)[0]()

    def x_first(j):
        x_ring(j)[1](2)

    def x_second(j):
        total = x_ring(j)[2]()
        own[j] = total
        zs[j] = total.astype(BF16).reshape(NZ, NY, 16, CB)
        for d, e in owners:
            z_send(j, d, e).start()

    def z_start(i):
        weight_grad(ZB[i], True)
        z_ring(i)[0]()

    def z_last(i):
        total = z_ring(i)[2]()
        own[ZB[i], : NY * NX] = total
        xs[i] = total.astype(BF16).reshape(NY, NX, 16, CB)
        for d, e in x_owners:
            xo_send(i, d, e).start()

    def x_sum(i):
        landed(xr.at[i, pl.ds(1, NX * NY - 1)], xo_r.at[i])
        total = own[ZB[i], yl * NX + x]
        for d, e in x_owners:
            total = total + xr[i, d * NY + e].astype(F32)
        to_core(ZB[i], total)

    def to_core(j, total):
        fs[0, j] = total[:8]
        fs[1, j] = total[8:]
        core_send(j).start()

    def xo_send(i, d, e):
        xp, yp = away(x, d, NX), away(yl, e, NY)
        return pltpu.make_async_remote_copy(
            src_ref=xs.at[i, yp, xp],
            dst_ref=xr.at[i, d * NY + e],
            send_sem=xo_s.at[i],
            recv_sem=xo_r.at[i],
            device_id={"dp_2": xp, "dp_1": yp},
            device_id_type=MESH,
        )

    def z_sum(j):
        landed(zr.at[j, pl.ds(1, ZY - 1)], z_r.at[j])
        total = own[j, z * NY + yl]
        for d, e in owners:
            total = total + zr[j, d * NY + e].astype(F32)
        to_core(j, total)

    def context_swap(k):
        return send(gcs.at[k], gcr.at[k], gc_s.at[0], gc_s.at[1], "dp_3", oc)

    def context_dots(k, blocks):
        rows = pl.ds(pl.multiple_of(k * QR, QR), QR)
        total = None
        for left_hand, b in blocks:
            term = dot_nt(left_hand, wv[b, rows, :])
            total = term if total is None else total + term
        return total

    def context_own(k):
        own_blocks = [(gaf[h, j, m], h * NB + j) for h in range(2) for j in range(NB)]
        gcv[k, m] = context_dots(k, own_blocks).astype(BF16)

    def context_grad(k):
        gcs[k] = context_dots(k, [(gas[j, om], c * NB + j) for j in range(NB)])
        context_swap(k).start()
        gcb[k] = context_dots(k, [(gaf[c, j, om], c * NB + j) for j in range(NB)])

    def context_join():
        landed(gcr, gc_s.at[1])
        for k in range(H // QR):
            gcv[k, om] = (gcb[k] + gcr[k]).astype(BF16)
            for who in range(2):
                pltpu.make_async_copy(
                    gcv.at[k, who],
                    gc_hbm.at[pl.ds(who * TH, TH), pl.ds(k * QR, QR)],
                    o_sem.at[4],
                ).start()

    steps_z = NZ // 2
    NK = H // QR
    per = max(1, NK // 2)
    stages = [(x_start, 0), (z_sum, 5), (x_second, 3), (x_first, 1)]
    z_stages = [z_start]
    z_stages += [lambda i, n=n: z_ring(i)[1](n) for n in range(2, steps_z + 1)]
    z_stages += [z_last, x_sum]
    gain_steps = (2, 3, NB - 1, NB + 2, NB + 4)
    last = max([NB + 5] + [b + Z_PLAN[b][steps_z + 1] + 1 for b in ZB])

    def step(t):
        for stage, lag in stages:
            mine = (t >= lag) & (t < NB + lag)
            for b in ZB:
                mine = mine & (t != b + lag)

            @pl.when(mine)
            def _():
                with jax.named_scope(stage.__name__):
                    stage(t - lag)

        for n, stage in enumerate(z_stages):
            for i, b in enumerate(ZB):

                @pl.when(t == b + Z_PLAN[b][n])
                def _():
                    with jax.named_scope(f"z{n}#b={b}"):
                        stage(i)

        for k, when in enumerate(gain_steps):

            @pl.when(t == when)
            def _():
                with jax.named_scope("gain_stage"):
                    gain_stage(k)

        @pl.when((t >= NB) & (t < NB + NK // per))
        def _():
            with jax.named_scope("context_grad"):
                each_block(per, lambda i: context_grad((t - NB) * per + i))

        @pl.when(t == NB + 2)
        def _():
            with jax.named_scope("context_join"):
                context_join()

    with jax.named_scope("context_own"):
        each_block(NK, context_own)
    each_block(last, step)

    gr[c] = fs[c]
    m1_load.wait()
    m2_load.wait()
    with jax.named_scope("core_wait"):
        landed(gr.at[oc], f_r.at[0])
    row = pl.multiple_of(((z * NY + yl) * NX + x) * 16, 16)
    for b in range(NB2):
        cols = slice(b * CB, (b + 1) * CB)
        g = gr[b // NB, b % NB]
        first = beta_one * m1v[:, cols] + (1.0 - beta_one) * g
        second = beta_two * m2v[:, cols] + (1.0 - beta_two) * g * g
        both = wv[b, pl.ds(row, 16), :].astype(F32)
        master = jnp.where(c == 0, both[:8], both[8:])
        n1_ref[:, cols] = first
        n2_ref[:, cols] = second
        nw_ref[:, cols] = (master - learn_rate * first / (jnp.sqrt(second) + adam_floor)).astype(BF16)

    outs = [
        pltpu.make_async_copy(a, b, o_sem.at[i])
        for i, (a, b) in enumerate([(nw_ref, nw_hbm), (n1_ref, n1_hbm), (n2_ref, n2_hbm), (gg_ref, gg_hbm)])
    ]
    for copy in outs:
        copy.start()

    ctx_swap().wait_send()
    landed(psend, p_s.at[0])
    for hop in hops:
        if hop[3] > 1:
            landed(hop[0].at[pl.ds(0, hop[3] - 1)], hop[4])

    landed(gaf.at[:, :, m], ga_s.at[0])
    landed(gaf.at[0, :, m], sa_s.at[0])
    landed(gcs, gc_s.at[0])
    landed(fs.at[oc], f_s.at[0])

    def drain(j):
        x_ring(j)[3]()
        landed(zr.at[j, pl.ds(1, ZY - 1)], z_s.at[j])

    for j in range(NB):
        if j not in ZB:
            drain(j)
    for i in range(len(ZB)):
        z_ring(i)[3]()
        landed(xr.at[i, pl.ds(1, NX * NY - 1)], xo_s.at[i])
    landed(gcv, o_sem.at[4])
    for copy in outs:
        copy.wait()


def deliver(*refs):
    n = (len(refs) - 1) // 3
    src, dst, held, sem = refs[:n], refs[n : 2 * n], refs[2 * n : 3 * n], refs[-1]
    into = [pltpu.make_async_copy(s, h, sem.at[i]) for i, (s, h) in enumerate(zip(src, held))]
    out = [pltpu.make_async_copy(h, d, sem.at[n + i]) for i, (h, d) in enumerate(zip(held, dst))]
    for copy in into:
        copy.start()
    for first, second in zip(into, out):
        first.wait()
        second.start()
    for copy in out:
        copy.wait()


def delivered(arrays):
    space = pl.BlockSpec(memory_space=pl.ANY)
    return pl.pallas_call(
        deliver,
        out_shape=[jax.ShapeDtypeStruct(a.shape, a.dtype) for a in arrays],
        in_specs=[space] * len(arrays),
        out_specs=[space] * len(arrays),
        scratch_shapes=[pltpu.VMEM(a.shape, a.dtype) for a in arrays]
        + [pltpu.SemaphoreType.DMA((2 * len(arrays),))],
        name="deliver",
    )(*arrays)


def per_device(sizes, block, context, out_weight, cotangent, norm_gain, first_moment, second_moment):
    NZ, NY, NX = sizes
    T, H = context.shape
    D = out_weight.shape[1]
    TH, CB = T // 2, block
    NB = D // (2 * CB)
    NB2 = 2 * NB
    ZY = NZ * NY
    NZB = len(z_blocks(NB))
    rows8 = (NB2 + 7) // 8 * 8
    dims = (NZ, NY, NX, TH, H, D, NB, CB)
    dma = pltpu.SemaphoreType.DMA
    scratch = [
        pltpu.VMEM((8, D), BF16),
        pltpu.VMEM((8, D), F32),
        pltpu.VMEM((8, D), F32),
        pltpu.VMEM((D,), F32),
        pltpu.VMEM((H // QR, 2, TH, QR), BF16),
        pltpu.VMEM((H // QR, TH, QR), F32),
        pltpu.VMEM((H // QR, TH, QR), F32),
        pltpu.VMEM((H // QR, TH, QR), F32),
        pltpu.VMEM((2, TH, H), BF16),
        pltpu.VMEM((2, TH, H), BF16),
        pltpu.VMEM((NB2, H, CB), BF16),
        pltpu.VMEM((TH, D), BF16),
        pltpu.VMEM((NB2, TH, CB), F32),
        pltpu.VMEM((NB2, TH, CB), BF16),
        pltpu.VMEM((NB2, TH, CB), BF16),
        pltpu.VMEM((TH, 128), F32),
        pltpu.VMEM((TH, 128), F32),
        pltpu.VMEM((2, NB, 2, TH, CB), BF16),
        pltpu.VMEM((NB, 2, TH, CB), BF16),
        pltpu.VMEM((NB, NZ * NY * NX, 16, CB), F32),
        pltpu.VMEM((NB, max(ZY, NY * NX), 16, CB), F32),
        pltpu.VMEM((NB, (NX - 1) * ZY, 16, CB), BF16),
        pltpu.VMEM((NZB, (NZ - 1) * NY * NX, 16, CB), BF16),
        pltpu.VMEM((NB, NX // 2, 2, ZY, 16, CB), BF16),
        pltpu.VMEM((NZB, NZ // 2, 2, NY * NX, 16, CB), BF16),
        pltpu.VMEM((NB, NZ, NY, 16, CB), BF16),
        pltpu.VMEM((NB, ZY, 16, CB), BF16),
        pltpu.VMEM((NZB, NY, NX, 16, CB), BF16),
        pltpu.VMEM((NZB, NX * NY, 16, CB), BF16),
        pltpu.VMEM((2, NB, 8, CB), F32),
        pltpu.VMEM((2, NB, 8, CB), F32),
        pltpu.VMEM((8, D), F32),
        pltpu.VMEM((8, D), F32),
        pltpu.VMEM((NZ, rows8, CB), F32),
        pltpu.VMEM((NX, rows8, CB), F32),
        pltpu.VMEM((NY, rows8, CB), F32),
        pltpu.VMEM((2, rows8, CB), F32),
        pltpu.VMEM((2, rows8, CB), F32),
        dma((NB2,)), dma((5,)), dma((2,)),
        dma((1,)), dma((NB2 + 1,)),
        dma((1,)), dma((NB,)),
        dma((1,)), dma((NB,)),
        dma((NB,)), dma((NB, NX // 2)),
        dma((NZB,)), dma((NZB, NZ // 2)),
        dma((NB,)), dma((NB,)),
        dma((NZB,)), dma((NZB,)),
        dma((5,)),
        dma((1,)), dma((1,)),
        dma((5,)), dma((5,)),
        dma((2,)),
    ]
    any_space = pl.BlockSpec(memory_space=pl.ANY)
    vmem = pl.BlockSpec(memory_space=pltpu.VMEM)
    results = pl.pallas_call(
        functools.partial(kernel, dims),
        out_shape=[
            jax.ShapeDtypeStruct((8, D), BF16),
            jax.ShapeDtypeStruct((8, D), F32),
            jax.ShapeDtypeStruct((8, D), F32),
            jax.ShapeDtypeStruct((D,), F32),
            jax.ShapeDtypeStruct((T, H), BF16),
        ],
        in_specs=[any_space, any_space, any_space, vmem, any_space, any_space],
        out_specs=[any_space] * 5,
        scratch_shapes=scratch,
        compiler_params=pltpu.CompilerParams(
            collective_id=0, has_side_effects=True, vmem_limit_bytes=60 * 1024 * 1024
        ),
        name="step",
    )(context, out_weight, cotangent, norm_gain, first_moment[0], second_moment[0])
    nw, n1, n2, gg, gc = delivered(results)
    return (nw[None], n1[None], n2[None], gg, gc)


def build(finer, block):
    sizes = tuple(finer.shape[a] for a in ("dp_0", "dp_1", "dp_2"))
    placed = (P(DP, "mp"), P("mp", None), P(DP, None), P(), P("mp", DP, None), P("mp", DP, None))
    return jax.shard_map(
        functools.partial(per_device, sizes, block),
        mesh=finer,
        in_specs=placed,
        out_specs=(P("mp", DP, None), P("mp", DP, None), P("mp", DP, None), P(), P(DP, "mp")),
        check_vma=False,
    )


def solution(mesh):
    finer = Mesh(
        mesh.devices.reshape(8, 2, 4, 2, mesh.shape["mp"]), ("dp_0", "dp_1", "dp_2", "dp_3", "mp")
    )
    return build(finer, 256)
```

```python
import functools

import jax
import jax.numpy as jnp
from jax import lax
from jax.experimental import pallas as pl
from jax.experimental.pallas import tpu as pltpu
from jax.sharding import Mesh
from jax.sharding import PartitionSpec as P

DP = ("dp_0", "dp_1", "dp_2", "dp_3")
MESH = pl.DeviceIdType.MESH
F32 = jnp.float32
BF16 = jnp.bfloat16

norm_floor = 0.1
learn_rate = 0.01
beta_one = 0.9
beta_two = 0.95
adam_floor = 1e-08

QR = 256


Z_PLAN = {0: (0, 1, 3, 5, 7, 9), 1: (0, 1, 3, 5, 7, 9), 3: (0, 1, 2, 3, 5, 7)}


AHEAD = 2


def z_blocks(n):
    return [b for b in Z_PLAN if b < n - 1]


def far_first(n):
    return sorted(range(n), key=lambda d: -min(d, n - d))


def dot_nn(a, b):
    return lax.dot_general(a, b, (((1,), (0,)), ((), ())), preferred_element_type=F32)


def dot_tn(a, b):
    return lax.dot_general(a, b, (((0,), (0,)), ((), ())), preferred_element_type=F32)


def dot_nt(a, b):
    return lax.dot_general(a, b, (((1,), (1,)), ((), ())), preferred_element_type=F32)


def send(src, dst, send_sem, recv_sem, axis, peer):
    return pltpu.make_async_remote_copy(
        src_ref=src,
        dst_ref=dst,
        send_sem=send_sem,
        recv_sem=recv_sem,
        device_id={axis: peer},
        device_id_type=MESH,
    )


def landed(ref, sem):
    pltpu.make_async_copy(ref, ref, sem).wait()


def kernel(
    dims,
    ctx_hbm, w_hbm, cot_hbm, gain_ref,
    g_hbm, gg_hbm, gc_hbm,
    gg_ref, gcv, gcs, gcr, gcb,
    ctx_o, ctx_s, wv, cot, att, psend, precv, ssr, spr, gaf, gas,
    grad, own, ox, oz, rx, rz, zs, zr, xs, xr, fs, gz, gx, gy, gm, gk,
    ld_w, ld, c_sem, p_s, p_r, ga_s, ga_r, sa_s, sa_r, x_s, x_r, zz_s, zz_r,
    z_s, z_r, xo_s, xo_r, o_sem, f_s, f_r, gt_s, gt_r, gc_s,
):
    NZ, NY, NX, TH, H, D, NB, CB = dims
    ZB = z_blocks(NB)
    NG = NZ * NY * NX
    TA = TH * 4 // 5 // 16 * 16
    NB2 = 2 * NB
    ZY = NZ * NY
    T = 2 * TH
    z = lax.axis_index("dp_0")
    yl = lax.axis_index("dp_1")
    x = lax.axis_index("dp_2")
    c = lax.axis_index("dp_3")
    m = lax.axis_index("mp")

    def away(me, d, n):
        return lax.rem(me + d, n)

    om, oc = 1 - m, 1 - c
    owners = [(d, e) for d in far_first(NZ) for e in far_first(NY) if (d, e) != (0, 0)]
    x_owners = [(d, e) for d in far_first(NX) for e in far_first(NY) if (d, e) != (0, 0)]

    def each_block(n, body):
        def step(i, carry):
            body(i)
            return carry

        lax.fori_loop(0, n, step, 0)

    barrier = pltpu.get_barrier_semaphore()
    peers = [{"dp_3": oc}, {"mp": om}, {"mp": om, "dp_3": oc}]
    peers += [{"dp_2": away(x, d, NX), "dp_1": away(yl, e, NY)} for d, e in x_owners if d]
    peers += [{"dp_0": away(z, d, NZ), "dp_1": away(yl, e, NY)} for d, e in owners]
    for peer in peers:
        pl.semaphore_signal(barrier, inc=1, device_id=peer, device_id_type=MESH)
    ctx_loads = [
        pltpu.make_async_copy(ctx_hbm.at[pl.ds(k * TH, TH), :], ctx_o.at[k], ld.at[k]) for k in range(2)
    ]
    cot_load = pltpu.make_async_copy(
        cot_hbm.at[pl.ds(pl.multiple_of(m * TH, TH), TH), :], cot, ld.at[2]
    )

    def w_load(b):
        return pltpu.make_async_copy(
            w_hbm.at[:, pl.ds(pl.multiple_of(b * CB, CB), CB)], wv.at[b], ld_w.at[b]
        )

    for copy in ctx_loads:
        copy.start()
    each_block(NB2, lambda b: w_load(b).start())
    cot_load.start()

    with jax.named_scope("greet"):
        pl.semaphore_wait(barrier, len(peers))

    with jax.named_scope("ctx_wait"):
        for copy in ctx_loads:
            copy.wait()

    def ctx_swap():
        return send(ctx_o, ctx_s, c_sem.at[0], c_sem.at[1], "dp_3", oc)

    ctx_swap().start()

    head, tail = slice(0, TA), slice(TA, TH)

    def partial_send(b):
        return send(psend.at[b, head], precv.at[b, head], p_s.at[0], p_r.at[b], "mp", om)

    def partial_rest():
        return send(psend.at[:, tail], precv.at[:, tail], p_s.at[0], p_r.at[NB2], "mp", om)

    def project_theirs(b):
        w_load(b).wait()
        psend[b] = dot_nn(ctx_o[om], wv[b]).astype(BF16)
        partial_send(b).start()

    with jax.named_scope("project_theirs"):
        each_block(NB2, project_theirs)

    partial_rest().start()
    cot_load.wait()
    ssr[...] = jnp.zeros_like(ssr)
    spr[...] = jnp.zeros_like(spr)
    gz[z] = jnp.zeros(gz.shape[1:], F32)

    def columns(b):
        return pl.ds(pl.multiple_of(b * CB, CB), CB)

    def project_ours(b):
        att[b] = dot_nn(ctx_o[m], wv[b])

    with jax.named_scope("project_ours"):
        each_block(NB2, project_ours)

    def add_theirs(b, rows):
        a = att[b, rows] + precv[b, rows].astype(F32)
        att[b, rows] = a
        s = cot[rows, columns(b)].astype(F32) * gain_ref[columns(b)][None, :]
        sq, pr = a * a, a * s
        for k in range(CB // 128):
            ssr[rows] += sq[:, k * 128 : (k + 1) * 128]
            spr[rows] += pr[:, k * 128 : (k + 1) * 128]

    def add_head(b):
        with jax.named_scope("wait_partial"):
            partial_send(b).wait_recv()
        add_theirs(b, head)

    with jax.named_scope("add_head"):
        each_block(NB2, add_head)

    def row_terms(rows):
        inverse = lax.rsqrt(jnp.sum(ssr[rows], axis=1, keepdims=True) / D + norm_floor)
        return inverse, inverse * (jnp.sum(spr[rows], axis=1, keepdims=True) / D)

    def ga_sends(j, rows):
        here, there = gaf.at[c, j, m, rows], gaf.at[oc, j, m, rows]
        straight = send(here, here, ga_s.at[0], ga_r.at[j], "mp", om)
        crossed = pltpu.make_async_remote_copy(
            src_ref=there,
            dst_ref=gas.at[j, m, rows],
            send_sem=ga_s.at[0],
            recv_sem=sa_r.at[j],
            device_id={"mp": om, "dp_3": oc},
            device_id_type=MESH,
        )
        return straight, crossed

    def side_send(j):
        return send(gaf.at[oc, j, m], gas.at[j, m], sa_s.at[0], sa_r.at[j], "dp_3", oc)

    def norm_gradient(j, rows, terms):
        inverse, mean_sn = terms
        for h in range(2):
            b = h * NB + j
            u = cot[rows, columns(b)].astype(F32)
            s = u * gain_ref[columns(b)][None, :]
            normed = att[b, rows] * inverse
            gaf[h, j, m, rows] = (inverse * (s - normed * mean_sn)).astype(BF16)
            gz[z, pl.ds(b, 1), :] += jnp.sum(u * normed, axis=0, keepdims=True)
        for copy in ga_sends(j, rows):
            copy.start()

    head_terms = row_terms(head)
    with jax.named_scope("norm_head"):
        each_block(AHEAD, lambda j: norm_gradient(j, head, head_terms))
    with jax.named_scope("add_tail"):
        partial_rest().wait_recv()
        each_block(NB2, lambda b: add_theirs(b, tail))
    tail_terms = row_terms(tail)

    def norm_tail(j):
        norm_gradient(j, tail, tail_terms)
        side_send(j).start()

    def norm_both(j):
        norm_gradient(j, head, head_terms)
        norm_tail(j)

    with jax.named_scope("norm_tail"):
        each_block(AHEAD, norm_tail)
        each_block(NB - AHEAD, lambda j: norm_both(j + AHEAD))

    def gain_hop(buf, axis, me, n, ss, rs):
        return [
            send(buf.at[me], buf.at[me], ss, rs, axis, away(me, d, n)) for d in range(1, n)
        ]

    def gain_wait(buf, axis, me, n, ss, rs):
        if n > 1:
            landed(buf.at[pl.ds(0, n - 1)], rs)

    hops = [
        (gz, "dp_0", z, NZ, gt_s.at[0], gt_r.at[0]),
        (gx, "dp_2", x, NX, gt_s.at[1], gt_r.at[1]),
        (gy, "dp_1", yl, NY, gt_s.at[2], gt_r.at[2]),
        (gm, "mp", m, 2, gt_s.at[3], gt_r.at[3]),
        (gk, "dp_3", c, 2, gt_s.at[4], gt_r.at[4]),
    ]

    def summed(buf, n):
        total = buf[0]
        for i in range(1, n):
            total = total + buf[i]
        return total

    for copy in gain_hop(*hops[0]):
        copy.start()

    def gain_stage(k):
        buf, _, _, n, _, _ = hops[k]
        gain_wait(*hops[k])
        total = summed(buf, n)
        if k + 1 < len(hops):
            nxt = hops[k + 1]
            nxt[0][nxt[2]] = total
            for copy in gain_hop(*nxt):
                copy.start()
        else:
            for b in range(NB2):
                gg_ref[b * CB : (b + 1) * CB] = total[b]

    ctx_swap().wait_recv()

    def ring(j, out, buf, n, me, axis, ss, rs, size, stride, base):
        steps = n // 2
        half = size // 2

        def target(t, k):
            far = steps + 1 - t
            return away(me, far if k == 0 else n - far, n) * stride + base

        def out_rows(t, k):
            if t == 1:
                return pl.ds(k * half, half)
            return pl.ds(size + (t - 2) * 2 * size + k * size, size)

        def hop(t, k):
            peer = away(me, 1 if k == 0 else n - 1, n)
            dst = buf(t - 1, k, pl.ds(0, half)) if t == 1 else buf(t - 1, k, pl.ds(0, size))
            return send(out(out_rows(t, k)), dst, ss, rs(t - 1), axis, peer)

        def arrived(t, k):
            return buf(t - 1, k, pl.ds(0, half if t == 1 else size))[...].astype(F32)

        def wait(t):
            landed(buf(t - 1, slice(None), pl.ds(0, half if t == 1 else size)), rs(t - 1))

        def start():
            for k in range(2):
                out(out_rows(1, k))[...] = grad[j, pl.ds(target(1, k) + k * half, half)].astype(BF16)
            for k in range(2):
                hop(1, k).start()

        def add_and_start(t):
            wait(t - 1)
            for k in range(2):
                at = target(t, k)
                if t == 2:
                    at_out = size + k * size
                    mine, other = k * half, (1 - k) * half
                    total = grad[j, pl.ds(at + mine, half)] + arrived(1, k)
                    out(pl.ds(at_out + mine, half))[...] = total.astype(BF16)
                    rest = grad[j, pl.ds(at + other, half)]
                    out(pl.ds(at_out + other, half))[...] = rest.astype(BF16)
                else:
                    total = grad[j, pl.ds(at, size)] + arrived(t - 1, k)
                    out(out_rows(t, k))[...] = total.astype(BF16)
            for k in range(2):
                hop(t, k).start()

        def total():
            wait(steps)
            return grad[j, pl.ds(me * stride + base, size)] + arrived(steps, 0) + arrived(steps, 1)

        def sent():
            landed(out(pl.ds(0, (2 * steps - 1) * size)), ss)

        return start, add_and_start, total, sent

    def x_ring(j, r):
        at = (1 - yl if r == 0 else yl) * NZ
        return ring(
            j,
            lambda rows: ox.at[j, r, rows],
            lambda t, k, rows: rx.at[j, r, t, k, rows],
            NX, x, "dp_2", x_s.at[j, r], lambda t: x_r.at[j, r, t], NZ, ZY, at,
        )

    def z_ring(i):
        return ring(
            ZB[i],
            lambda rows: oz.at[i, rows],
            lambda t, k, rows: rz.at[i, t, k, rows],
            NZ, z, "dp_0", zz_s.at[i], lambda t: zz_r.at[i, t], NX * NY, NX * NY, 0,
        )

    def z_send(j, d, e):
        zp, yp = away(z, d, NZ), away(yl, e, NY)
        return pltpu.make_async_remote_copy(
            src_ref=zs.at[j, yp, zp],
            dst_ref=zr.at[j, d * NY + e],
            send_sem=z_s.at[j],
            recv_sem=z_r.at[j],
            device_id={"dp_0": zp, "dp_1": yp},
            device_id_type=MESH,
        )

    def core_send(j):
        return send(fs.at[oc, j], g_hbm.at[c, j], f_s.at[0], f_r.at[0], "dp_3", oc)

    def weight_grad(j, z_first):
        landed(gaf.at[c, j, om], ga_r.at[j])
        landed(gas.at[j], sa_r.at[j])
        ours = gaf[c, j].reshape(T, CB)
        theirs = gas[j].reshape(T, CB)
        per = QR // 16
        for q in range(H // QR):
            cols = slice(q * QR, (q + 1) * QR)
            part = dot_tn(ctx_o[:, :, cols].reshape(T, QR), ours)
            part = part + dot_tn(ctx_s[:, :, cols].reshape(T, QR), theirs)
            if z_first:
                grad[j, q * per : (q + 1) * per] = part.reshape(per, 16, CB)
            else:
                zq = per // (NX * NY)
                part = part.reshape(zq, NY, NX, 16, CB)
                for k in range(NX):
                    for e in range(NY):
                        at = k * ZY + e * NZ + q * zq
                        grad[j, at : at + zq] = part[:, e, k]

    def x_start(j):
        weight_grad(j, False)
        for r in range(2):
            x_ring(j, r)[0]()

    def x_first(j):
        for r in range(2):
            x_ring(j, r)[1](2)

    def x_second(j):
        for r in range(2):
            side = 1 - yl if r == 0 else yl
            total = x_ring(j, r)[2]()
            own[j, pl.ds(side * NZ, NZ)] = total
            zs[j, side] = total.astype(BF16)
            for d, e in owners:
                if (e == 0) == (r == 1):
                    z_send(j, d, e).start()

    def z_start(i):
        weight_grad(ZB[i], True)
        z_ring(i)[0]()

    def z_last(i):
        total = z_ring(i)[2]()
        own[ZB[i], : NY * NX] = total
        xs[i] = total.astype(BF16).reshape(NY, NX, 16, CB)
        for d, e in x_owners:
            xo_send(i, d, e).start()

    def x_sum(i):
        landed(xr.at[i, pl.ds(1, NX * NY - 1)], xo_r.at[i])
        total = own[ZB[i], yl * NX + x]
        for d, e in x_owners:
            total = total + xr[i, d * NY + e].astype(F32)
        to_core(ZB[i], total)

    def to_core(j, total):
        fs[0, j] = total[:8]
        fs[1, j] = total[8:]
        core_send(j).start()
        pltpu.make_async_copy(fs.at[c, j], g_hbm.at[c, j], o_sem.at[1]).start()

    def xo_send(i, d, e):
        xp, yp = away(x, d, NX), away(yl, e, NY)
        return pltpu.make_async_remote_copy(
            src_ref=xs.at[i, yp, xp],
            dst_ref=xr.at[i, d * NY + e],
            send_sem=xo_s.at[i],
            recv_sem=xo_r.at[i],
            device_id={"dp_2": xp, "dp_1": yp},
            device_id_type=MESH,
        )

    def z_sum(j):
        landed(zr.at[j, pl.ds(1, ZY - 1)], z_r.at[j])
        total = own[j, yl * NZ + z]
        for d, e in owners:
            total = total + zr[j, d * NY + e].astype(F32)
        to_core(j, total)

    def context_swap(k):
        return send(gcs.at[k], gcr.at[k], gc_s.at[0], gc_s.at[1], "dp_3", oc)

    def context_dots(k, blocks):
        rows = pl.ds(pl.multiple_of(k * QR, QR), QR)
        total = None
        for left_hand, b in blocks:
            term = dot_nt(left_hand, wv[b, rows, :])
            total = term if total is None else total + term
        return total

    def context_own(k):
        own_blocks = [(gaf[h, j, m], h * NB + j) for h in range(2) for j in range(NB)]
        gcv[k, m] = context_dots(k, own_blocks).astype(BF16)

    def context_grad(k):
        gcs[k] = context_dots(k, [(gas[j, om], c * NB + j) for j in range(NB)])
        context_swap(k).start()
        gcb[k] = context_dots(k, [(gaf[c, j, om], c * NB + j) for j in range(NB)])

    def context_join():
        landed(gcr, gc_s.at[1])
        for k in range(H // QR):
            gcv[k, om] = (gcb[k] + gcr[k]).astype(BF16)
            for who in range(2):
                pltpu.make_async_copy(
                    gcv.at[k, who],
                    gc_hbm.at[pl.ds(who * TH, TH), pl.ds(k * QR, QR)],
                    o_sem.at[4],
                ).start()

    steps_z = NZ // 2
    NK = H // QR
    per = max(1, NK // 2)
    stages = [(x_start, 0), (z_sum, 6), (x_second, 3), (x_first, 1)]
    z_stages = [z_start]
    z_stages += [lambda i, n=n: z_ring(i)[1](n) for n in range(2, steps_z + 1)]
    z_stages += [z_last, x_sum]
    gain_steps = (2, 3, NB - 1, NB + 2, NB + 5)
    last = max([NB + 6] + [b + Z_PLAN[b][steps_z + 1] + 1 for b in ZB])

    def step(t):
        for stage, lag in stages:
            mine = (t >= lag) & (t < NB + lag)
            if stage is x_second:
                mine = mine & (t != NB - 1 + lag)
            for b in ZB:
                mine = mine & (t != b + lag)

            @pl.when(mine)
            def _():
                with jax.named_scope(stage.__name__):
                    stage(t - lag)

        @pl.when(t == NB + 1)
        def _():
            with jax.named_scope("x_second_last"):
                x_second(NB - 1)

        for n, stage in enumerate(z_stages):
            for i, b in enumerate(ZB):

                @pl.when(t == b + Z_PLAN[b][n])
                def _():
                    with jax.named_scope(f"z{n}#b={b}"):
                        stage(i)

        for k, when in enumerate(gain_steps):

            @pl.when(t == when)
            def _():
                with jax.named_scope("gain_stage"):
                    gain_stage(k)

        @pl.when((t >= NB) & (t < NB + NK // per))
        def _():
            with jax.named_scope("context_grad"):
                each_block(per, lambda i: context_grad((t - NB) * per + i))

        @pl.when(t == NB + 2)
        def _():
            with jax.named_scope("context_join"):
                context_join()

    with jax.named_scope("context_own"):
        each_block(NK, context_own)
    each_block(last, step)

    gain_out = pltpu.make_async_copy(gg_ref, gg_hbm, o_sem.at[0])
    gain_out.start()
    with jax.named_scope("core_wait"):
        landed(g_hbm.at[oc], f_r.at[0])

    ctx_swap().wait_send()
    landed(psend, p_s.at[0])
    for hop in hops:
        if hop[3] > 1:
            landed(hop[0].at[pl.ds(0, hop[3] - 1)], hop[4])

    landed(gaf.at[:, :, m], ga_s.at[0])
    landed(gaf.at[0, :, m], sa_s.at[0])
    landed(gcs, gc_s.at[0])
    landed(fs.at[oc], f_s.at[0])

    def drain(j):
        for r in range(2):
            x_ring(j, r)[3]()
        landed(zr.at[j, pl.ds(1, ZY - 1)], z_s.at[j])

    for j in range(NB):
        if j not in ZB:
            drain(j)
    for i in range(len(ZB)):
        z_ring(i)[3]()
        landed(xr.at[i, pl.ds(1, NX * NY - 1)], xo_s.at[i])
    landed(gcv, o_sem.at[4])
    landed(g_hbm.at[c], o_sem.at[1])
    gain_out.wait()


def deliver(
    dims,
    g_hbm, gg_hbm, gc_hbm, w_hbm, m1_hbm, m2_hbm,
    nw_hbm, n1_hbm, n2_hbm, gg_out, gc_out,
    gv, ggv, gcv, w16, m1v, m2v, nwv, n1v, n2v, sem,
):
    NZ, NY, NX, TH, H, D, NB, CB = dims
    z, yl, x, c = (lax.axis_index(a) for a in DP)
    row = pl.multiple_of(((z * NY + yl) * NX + x) * 16, 16)
    pairs = [(gc_hbm, gcv), (gg_hbm, ggv), (g_hbm, gv), (w_hbm.at[pl.ds(row, 16), :], w16), (m1_hbm, m1v), (m2_hbm, m2v)]
    into = [pltpu.make_async_copy(a, b, sem.at[i]) for i, (a, b) in enumerate(pairs)]
    pairs = [(gcv, gc_out), (ggv, gg_out), (nwv, nw_hbm), (n1v, n1_hbm), (n2v, n2_hbm)]
    out = [pltpu.make_async_copy(a, b, sem.at[6 + i]) for i, (a, b) in enumerate(pairs)]
    for copy in into:
        copy.start()
    for i in range(2):
        into[i].wait()
        out[i].start()
    for copy in into[2:]:
        copy.wait()
    for b in range(2 * NB):
        cols = slice(b * CB, (b + 1) * CB)
        g = gv[b // NB, b % NB]
        first = beta_one * m1v[:, cols] + (1.0 - beta_one) * g
        second = beta_two * m2v[:, cols] + (1.0 - beta_two) * g * g
        both = w16[:, cols].astype(F32)
        master = jnp.where(c == 0, both[:8], both[8:])
        n1v[:, cols] = first
        n2v[:, cols] = second
        nwv[:, cols] = (master - learn_rate * first / (jnp.sqrt(second) + adam_floor)).astype(BF16)
    for copy in out[2:]:
        copy.start()
    for copy in out:
        copy.wait()


def per_device(sizes, block, context, out_weight, cotangent, norm_gain, first_moment, second_moment):
    NZ, NY, NX = sizes
    T, H = context.shape
    D = out_weight.shape[1]
    TH, CB = T // 2, block
    NB = D // (2 * CB)
    NB2 = 2 * NB
    ZY = NZ * NY
    NZB = len(z_blocks(NB))
    rows8 = (NB2 + 7) // 8 * 8
    dims = (NZ, NY, NX, TH, H, D, NB, CB)
    dma = pltpu.SemaphoreType.DMA
    scratch = [
        pltpu.VMEM((D,), F32),
        pltpu.VMEM((H // QR, 2, TH, QR), BF16),
        pltpu.VMEM((H // QR, TH, QR), F32),
        pltpu.VMEM((H // QR, TH, QR), F32),
        pltpu.VMEM((H // QR, TH, QR), F32),
        pltpu.VMEM((2, TH, H), BF16),
        pltpu.VMEM((2, TH, H), BF16),
        pltpu.VMEM((NB2, H, CB), BF16),
        pltpu.VMEM((TH, D), BF16),
        pltpu.VMEM((NB2, TH, CB), F32),
        pltpu.VMEM((NB2, TH, CB), BF16),
        pltpu.VMEM((NB2, TH, CB), BF16),
        pltpu.VMEM((TH, 128), F32),
        pltpu.VMEM((TH, 128), F32),
        pltpu.VMEM((2, NB, 2, TH, CB), BF16),
        pltpu.VMEM((NB, 2, TH, CB), BF16),
        pltpu.VMEM((NB, NZ * NY * NX, 16, CB), F32),
        pltpu.VMEM((NB, max(ZY, NY * NX), 16, CB), F32),
        pltpu.VMEM((NB, 2, (NX - 1) * NZ, 16, CB), BF16),
        pltpu.VMEM((NZB, (NZ - 1) * NY * NX, 16, CB), BF16),
        pltpu.VMEM((NB, 2, NX // 2, 2, NZ, 16, CB), BF16),
        pltpu.VMEM((NZB, NZ // 2, 2, NY * NX, 16, CB), BF16),
        pltpu.VMEM((NB, NY, NZ, 16, CB), BF16),
        pltpu.VMEM((NB, ZY, 16, CB), BF16),
        pltpu.VMEM((NZB, NY, NX, 16, CB), BF16),
        pltpu.VMEM((NZB, NX * NY, 16, CB), BF16),
        pltpu.VMEM((2, NB, 8, CB), F32),
        pltpu.VMEM((NZ, rows8, CB), F32),
        pltpu.VMEM((NX, rows8, CB), F32),
        pltpu.VMEM((NY, rows8, CB), F32),
        pltpu.VMEM((2, rows8, CB), F32),
        pltpu.VMEM((2, rows8, CB), F32),
        dma((NB2,)), dma((5,)), dma((2,)),
        dma((1,)), dma((NB2 + 1,)),
        dma((1,)), dma((NB,)),
        dma((1,)), dma((NB,)),
        dma((NB, 2)), dma((NB, 2, NX // 2)),
        dma((NZB,)), dma((NZB, NZ // 2)),
        dma((NB,)), dma((NB,)),
        dma((NZB,)), dma((NZB,)),
        dma((5,)),
        dma((1,)), dma((1,)),
        dma((5,)), dma((5,)),
        dma((2,)),
    ]
    any_space = pl.BlockSpec(memory_space=pl.ANY)
    vmem = pl.BlockSpec(memory_space=pltpu.VMEM)
    g, gg, gc = pl.pallas_call(
        functools.partial(kernel, dims),
        out_shape=[
            jax.ShapeDtypeStruct((2, NB, 8, CB), F32),
            jax.ShapeDtypeStruct((D,), F32),
            jax.ShapeDtypeStruct((T, H), BF16),
        ],
        in_specs=[any_space, any_space, any_space, vmem],
        out_specs=[any_space] * 3,
        scratch_shapes=scratch,
        compiler_params=pltpu.CompilerParams(
            collective_id=0, has_side_effects=True, vmem_limit_bytes=60 * 1024 * 1024
        ),
        name="step",
    )(context, out_weight, cotangent, norm_gain)
    shard = jax.ShapeDtypeStruct((8, D), F32)
    results = [jax.ShapeDtypeStruct((8, D), BF16), shard, shard, jax.ShapeDtypeStruct((D,), F32)]
    results.append(jax.ShapeDtypeStruct((T, H), BF16))
    moved = [(2, NB, 8, CB), (D,), (T, H), (16, D), (8, D), (8, D), (8, D), (8, D), (8, D)]
    types = [F32, F32, BF16, BF16, F32, F32, BF16, F32, F32]
    nw, n1, n2, gg, gc = pl.pallas_call(
        functools.partial(deliver, dims),
        out_shape=results,
        in_specs=[any_space] * 6,
        out_specs=[any_space] * 5,
        scratch_shapes=[pltpu.VMEM(a, b) for a, b in zip(moved, types)] + [dma((11,))],
        compiler_params=pltpu.CompilerParams(vmem_limit_bytes=60 * 1024 * 1024),
        name="deliver",
    )(g, gg, gc, out_weight, first_moment[0], second_moment[0])
    return (nw[None], n1[None], n2[None], gg, gc)


def build(finer, block):
    sizes = tuple(finer.shape[a] for a in ("dp_0", "dp_1", "dp_2"))
    placed = (P(DP, "mp"), P("mp", None), P(DP, None), P(), P("mp", DP, None), P("mp", DP, None))
    return jax.shard_map(
        functools.partial(per_device, sizes, block),
        mesh=finer,
        in_specs=placed,
        out_specs=(P("mp", DP, None), P("mp", DP, None), P("mp", DP, None), P(), P(DP, "mp")),
        check_vma=False,
    )


def solution(mesh):
    finer = Mesh(
        mesh.devices.reshape(8, 2, 4, 2, mesh.shape["mp"]), ("dp_0", "dp_1", "dp_2", "dp_3", "mp")
    )
    return build(finer, 256)
```

```python
import functools

import jax
import jax.numpy as jnp
from jax import lax
from jax.experimental import pallas as pl
from jax.experimental.pallas import tpu as pltpu
from jax.sharding import Mesh
from jax.sharding import PartitionSpec as P

DP = ("dp_0", "dp_1", "dp_2", "dp_3")
MESH = pl.DeviceIdType.MESH
F32 = jnp.float32
BF16 = jnp.bfloat16

norm_floor = 0.1
learn_rate = 0.01
beta_one = 0.9
beta_two = 0.95
adam_floor = 1e-08

QR = 256


Z_PLAN = {0: (0, 1, 3, 5, 7, 9), 1: (0, 1, 3, 5, 7, 9), 3: (0, 1, 2, 3, 5, 7)}


AHEAD = 2


def z_blocks(n):
    return [b for b in Z_PLAN if b < n - 1]


def far_first(n):
    return sorted(range(n), key=lambda d: -min(d, n - d))


def dot_nn(a, b):
    return lax.dot_general(a, b, (((1,), (0,)), ((), ())), preferred_element_type=F32)


def dot_tn(a, b):
    return lax.dot_general(a, b, (((0,), (0,)), ((), ())), preferred_element_type=F32)


def dot_nt(a, b):
    return lax.dot_general(a, b, (((1,), (1,)), ((), ())), preferred_element_type=F32)


def send(src, dst, send_sem, recv_sem, axis, peer):
    return pltpu.make_async_remote_copy(
        src_ref=src,
        dst_ref=dst,
        send_sem=send_sem,
        recv_sem=recv_sem,
        device_id={axis: peer},
        device_id_type=MESH,
    )


def landed(ref, sem):
    pltpu.make_async_copy(ref, ref, sem).wait()


def kernel(
    dims,
    ctx_hbm, w_hbm, cot_hbm, gain_ref,
    g_hbm, gg_hbm, gc_hbm,
    gg_ref, gcv, gcs, gcr, gcb,
    ctx_o, ctx_s, wv, cot, att, psend, precv, ssr, spr, gaf, gas,
    grad, own, ox, oz, rx, rz, zs, zr, xs, xr, fs, gz, gx, gy, gm, gk,
    ld_w, ld, c_sem, p_s, p_r, ga_s, ga_r, sa_s, sa_r, x_s, x_r, zz_s, zz_r,
    z_s, z_r, xo_s, xo_r, o_sem, f_s, f_r, gt_s, gt_r, gc_s,
):
    NZ, NY, NX, TH, H, D, NB, CB = dims
    ZB = z_blocks(NB)
    NG = NZ * NY * NX
    TA = TH * 4 // 5 // 16 * 16
    NB2 = 2 * NB
    ZY = NZ * NY
    T = 2 * TH
    z = lax.axis_index("dp_0")
    yl = lax.axis_index("dp_1")
    x = lax.axis_index("dp_2")
    c = lax.axis_index("dp_3")
    m = lax.axis_index("mp")

    def away(me, d, n):
        return lax.rem(me + d, n)

    om, oc = 1 - m, 1 - c
    owners = [(d, e) for d in far_first(NZ) for e in far_first(NY) if (d, e) != (0, 0)]
    x_owners = [(d, e) for d in far_first(NX) for e in far_first(NY) if (d, e) != (0, 0)]

    def each_block(n, body):
        def step(i, carry):
            body(i)
            return carry

        lax.fori_loop(0, n, step, 0)

    barrier = pltpu.get_barrier_semaphore()
    peers = [{"dp_3": oc}, {"mp": om}, {"mp": om, "dp_3": oc}]
    peers += [{"dp_2": away(x, d, NX), "dp_1": away(yl, e, NY)} for d, e in x_owners if d]
    peers += [{"dp_0": away(z, d, NZ), "dp_1": away(yl, e, NY)} for d, e in owners]
    for peer in peers:
        pl.semaphore_signal(barrier, inc=1, device_id=peer, device_id_type=MESH)
    ctx_loads = [
        pltpu.make_async_copy(ctx_hbm.at[pl.ds(k * TH, TH), :], ctx_o.at[k], ld.at[k]) for k in range(2)
    ]
    cot_load = pltpu.make_async_copy(
        cot_hbm.at[pl.ds(pl.multiple_of(m * TH, TH), TH), :], cot, ld.at[2]
    )

    def w_load(b):
        return pltpu.make_async_copy(
            w_hbm.at[:, pl.ds(pl.multiple_of(b * CB, CB), CB)], wv.at[b], ld_w.at[b]
        )

    for copy in ctx_loads:
        copy.start()
    each_block(NB2, lambda b: w_load(b).start())
    cot_load.start()

    with jax.named_scope("greet"):
        pl.semaphore_wait(barrier, len(peers))

    with jax.named_scope("ctx_wait"):
        for copy in ctx_loads:
            copy.wait()

    def ctx_swap():
        return send(ctx_o, ctx_s, c_sem.at[0], c_sem.at[1], "dp_3", oc)

    ctx_swap().start()

    head, tail = slice(0, TA), slice(TA, TH)

    def partial_send(b):
        return send(psend.at[b, head], precv.at[b, head], p_s.at[0], p_r.at[b], "mp", om)

    def partial_rest():
        return send(psend.at[:, tail], precv.at[:, tail], p_s.at[0], p_r.at[NB2], "mp", om)

    def project_theirs(b):
        w_load(b).wait()
        psend[b] = dot_nn(ctx_o[om], wv[b]).astype(BF16)
        partial_send(b).start()

    with jax.named_scope("project_theirs"):
        each_block(NB2, project_theirs)

    partial_rest().start()
    cot_load.wait()
    ssr[...] = jnp.zeros_like(ssr)
    spr[...] = jnp.zeros_like(spr)
    gz[z] = jnp.zeros(gz.shape[1:], F32)

    def columns(b):
        return pl.ds(pl.multiple_of(b * CB, CB), CB)

    def project_ours(b):
        att[b] = dot_nn(ctx_o[m], wv[b])

    with jax.named_scope("project_ours"):
        each_block(NB2, project_ours)

    def add_theirs(b, rows):
        a = att[b, rows] + precv[b, rows].astype(F32)
        att[b, rows] = a
        s = cot[rows, columns(b)].astype(F32) * gain_ref[columns(b)][None, :]
        sq, pr = a * a, a * s
        for k in range(CB // 128):
            ssr[rows] += sq[:, k * 128 : (k + 1) * 128]
            spr[rows] += pr[:, k * 128 : (k + 1) * 128]

    def add_head(b):
        with jax.named_scope("wait_partial"):
            partial_send(b).wait_recv()
        add_theirs(b, head)

    with jax.named_scope("add_head"):
        each_block(NB2, add_head)

    def row_terms(rows):
        inverse = lax.rsqrt(jnp.sum(ssr[rows], axis=1, keepdims=True) / D + norm_floor)
        return inverse, inverse * (jnp.sum(spr[rows], axis=1, keepdims=True) / D)

    def ga_sends(j, rows):
        here, there = gaf.at[c, j, m, rows], gaf.at[oc, j, m, rows]
        straight = send(here, here, ga_s.at[0], ga_r.at[j], "mp", om)
        crossed = pltpu.make_async_remote_copy(
            src_ref=there,
            dst_ref=gas.at[j, m, rows],
            send_sem=ga_s.at[0],
            recv_sem=sa_r.at[j],
            device_id={"mp": om, "dp_3": oc},
            device_id_type=MESH,
        )
        return straight, crossed

    def side_send(j):
        return send(gaf.at[oc, j, m], gas.at[j, m], sa_s.at[0], sa_r.at[j], "dp_3", oc)

    def norm_gradient(j, rows, terms):
        inverse, mean_sn = terms
        for h in range(2):
            b = h * NB + j
            u = cot[rows, columns(b)].astype(F32)
            s = u * gain_ref[columns(b)][None, :]
            normed = att[b, rows] * inverse
            gaf[h, j, m, rows] = (inverse * (s - normed * mean_sn)).astype(BF16)
            gz[z, pl.ds(b, 1), :] += jnp.sum(u * normed, axis=0, keepdims=True)
        for copy in ga_sends(j, rows):
            copy.start()

    head_terms = row_terms(head)
    with jax.named_scope("norm_head"):
        each_block(AHEAD, lambda j: norm_gradient(j, head, head_terms))
    with jax.named_scope("add_tail"):
        partial_rest().wait_recv()
        each_block(NB2, lambda b: add_theirs(b, tail))
    tail_terms = row_terms(tail)

    def norm_tail(j):
        norm_gradient(j, tail, tail_terms)
        side_send(j).start()

    def norm_both(j):
        norm_gradient(j, head, head_terms)
        norm_tail(j)

    with jax.named_scope("norm_tail"):
        each_block(AHEAD, norm_tail)
        each_block(NB - AHEAD, lambda j: norm_both(j + AHEAD))

    def gain_hop(buf, axis, me, n, ss, rs):
        return [
            send(buf.at[me], buf.at[me], ss, rs, axis, away(me, d, n)) for d in range(1, n)
        ]

    def gain_wait(buf, axis, me, n, ss, rs):
        if n > 1:
            landed(buf.at[pl.ds(0, n - 1)], rs)

    hops = [
        (gz, "dp_0", z, NZ, gt_s.at[0], gt_r.at[0]),
        (gx, "dp_2", x, NX, gt_s.at[1], gt_r.at[1]),
        (gy, "dp_1", yl, NY, gt_s.at[2], gt_r.at[2]),
        (gm, "mp", m, 2, gt_s.at[3], gt_r.at[3]),
        (gk, "dp_3", c, 2, gt_s.at[4], gt_r.at[4]),
    ]

    def summed(buf, n):
        total = buf[0]
        for i in range(1, n):
            total = total + buf[i]
        return total

    for copy in gain_hop(*hops[0]):
        copy.start()

    def gain_stage(k):
        buf, _, _, n, _, _ = hops[k]
        gain_wait(*hops[k])
        total = summed(buf, n)
        if k + 1 < len(hops):
            nxt = hops[k + 1]
            nxt[0][nxt[2]] = total
            for copy in gain_hop(*nxt):
                copy.start()
        else:
            for b in range(NB2):
                gg_ref[b * CB : (b + 1) * CB] = total[b]

    ctx_swap().wait_recv()

    def ring(j, out, buf, n, me, axis, ss, rs, size, stride, base):
        steps = n // 2
        half = size // 2

        def target(t, k):
            far = steps + 1 - t
            return away(me, far if k == 0 else n - far, n) * stride + base

        def out_rows(t, k):
            if t == 1:
                return pl.ds(k * half, half)
            return pl.ds(size + (t - 2) * 2 * size + k * size, size)

        def hop(t, k):
            peer = away(me, 1 if k == 0 else n - 1, n)
            dst = buf(t - 1, k, pl.ds(0, half)) if t == 1 else buf(t - 1, k, pl.ds(0, size))
            return send(out(out_rows(t, k)), dst, ss, rs(t - 1), axis, peer)

        def arrived(t, k):
            return buf(t - 1, k, pl.ds(0, half if t == 1 else size))[...].astype(F32)

        def wait(t):
            landed(buf(t - 1, slice(None), pl.ds(0, half if t == 1 else size)), rs(t - 1))

        def start():
            for k in range(2):
                out(out_rows(1, k))[...] = grad[j, pl.ds(target(1, k) + k * half, half)].astype(BF16)
            for k in range(2):
                hop(1, k).start()

        def add_and_start(t):
            wait(t - 1)
            for k in range(2):
                at = target(t, k)
                if t == 2:
                    at_out = size + k * size
                    mine, other = k * half, (1 - k) * half
                    total = grad[j, pl.ds(at + mine, half)] + arrived(1, k)
                    out(pl.ds(at_out + mine, half))[...] = total.astype(BF16)
                    rest = grad[j, pl.ds(at + other, half)]
                    out(pl.ds(at_out + other, half))[...] = rest.astype(BF16)
                else:
                    total = grad[j, pl.ds(at, size)] + arrived(t - 1, k)
                    out(out_rows(t, k))[...] = total.astype(BF16)
            for k in range(2):
                hop(t, k).start()

        def total():
            wait(steps)
            return grad[j, pl.ds(me * stride + base, size)] + arrived(steps, 0) + arrived(steps, 1)

        def sent():
            landed(out(pl.ds(0, (2 * steps - 1) * size)), ss)

        return start, add_and_start, total, sent

    def x_ring(j, r):
        at = (1 - yl if r == 0 else yl) * NZ
        return ring(
            j,
            lambda rows: ox.at[j, r, rows],
            lambda t, k, rows: rx.at[j, r, t, k, rows],
            NX, x, "dp_2", x_s.at[j, r], lambda t: x_r.at[j, r, t], NZ, ZY, at,
        )

    def z_ring(i):
        return ring(
            ZB[i],
            lambda rows: oz.at[i, rows],
            lambda t, k, rows: rz.at[i, t, k, rows],
            NZ, z, "dp_0", zz_s.at[i], lambda t: zz_r.at[i, t], NX * NY, NX * NY, 0,
        )

    def z_send(j, d, e):
        zp, yp = away(z, d, NZ), away(yl, e, NY)
        return pltpu.make_async_remote_copy(
            src_ref=zs.at[j, yp, zp],
            dst_ref=zr.at[j, d * NY + e],
            send_sem=z_s.at[j],
            recv_sem=z_r.at[j],
            device_id={"dp_0": zp, "dp_1": yp},
            device_id_type=MESH,
        )

    def core_send(j):
        return send(fs.at[oc, j], g_hbm.at[c, j], f_s.at[0], f_r.at[0], "dp_3", oc)

    def weight_grad(j, z_first):
        landed(gaf.at[c, j, om], ga_r.at[j])
        landed(gas.at[j], sa_r.at[j])
        ours = gaf[c, j].reshape(T, CB)
        theirs = gas[j].reshape(T, CB)
        per = QR // 16
        for q in range(H // QR):
            cols = slice(q * QR, (q + 1) * QR)
            part = dot_tn(ctx_o[:, :, cols].reshape(T, QR), ours)
            part = part + dot_tn(ctx_s[:, :, cols].reshape(T, QR), theirs)
            if z_first:
                grad[j, q * per : (q + 1) * per] = part.reshape(per, 16, CB)
            else:
                zq = per // (NX * NY)
                part = part.reshape(zq, NY, NX, 16, CB)
                for k in range(NX):
                    for e in range(NY):
                        at = k * ZY + e * NZ + q * zq
                        grad[j, at : at + zq] = part[:, e, k]

    def x_start(j):
        weight_grad(j, False)
        for r in range(2):
            x_ring(j, r)[0]()

    def x_first(j):
        for r in range(2):
            x_ring(j, r)[1](2)

    def x_second(j):
        for r in range(2):
            side = 1 - yl if r == 0 else yl
            total = x_ring(j, r)[2]()
            own[j, pl.ds(side * NZ, NZ)] = total
            zs[j, side] = total.astype(BF16)
            for d, e in owners:
                if (e == 0) == (r == 1):
                    z_send(j, d, e).start()

    def z_start(i):
        weight_grad(ZB[i], True)
        z_ring(i)[0]()

    def z_last(i):
        total = z_ring(i)[2]()
        own[ZB[i], : NY * NX] = total
        xs[i] = total.astype(BF16).reshape(NY, NX, 16, CB)
        for d, e in x_owners:
            xo_send(i, d, e).start()

    def x_sum(i):
        landed(xr.at[i, pl.ds(1, NX * NY - 1)], xo_r.at[i])
        total = own[ZB[i], yl * NX + x]
        for d, e in x_owners:
            total = total + xr[i, d * NY + e].astype(F32)
        to_core(ZB[i], total)

    def to_core(j, total):
        fs[0, j] = total[:8]
        fs[1, j] = total[8:]
        core_send(j).start()
        pltpu.make_async_copy(fs.at[c, j], g_hbm.at[c, j], o_sem.at[1]).start()

    def xo_send(i, d, e):
        xp, yp = away(x, d, NX), away(yl, e, NY)
        return pltpu.make_async_remote_copy(
            src_ref=xs.at[i, yp, xp],
            dst_ref=xr.at[i, d * NY + e],
            send_sem=xo_s.at[i],
            recv_sem=xo_r.at[i],
            device_id={"dp_2": xp, "dp_1": yp},
            device_id_type=MESH,
        )

    def z_sum(j):
        landed(zr.at[j, pl.ds(1, ZY - 1)], z_r.at[j])
        total = own[j, yl * NZ + z]
        for d, e in owners:
            total = total + zr[j, d * NY + e].astype(F32)
        to_core(j, total)

    def context_swap(k):
        return send(gcs.at[k], gcr.at[k], gc_s.at[0], gc_s.at[1], "dp_3", oc)

    def context_dots(k, blocks):
        rows = pl.ds(pl.multiple_of(k * QR, QR), QR)
        total = None
        for left_hand, b in blocks:
            term = dot_nt(left_hand, wv[b, rows, :])
            total = term if total is None else total + term
        return total

    def context_own(k):
        own_blocks = [(gaf[h, j, m], h * NB + j) for h in range(2) for j in range(NB)]
        gcv[k, m] = context_dots(k, own_blocks).astype(BF16)

    def context_grad(k):
        gcs[k] = context_dots(k, [(gas[j, om], c * NB + j) for j in range(NB)])
        context_swap(k).start()
        gcb[k] = context_dots(k, [(gaf[c, j, om], c * NB + j) for j in range(NB)])

    def context_join():
        landed(gcr, gc_s.at[1])
        for k in range(H // QR):
            gcv[k, om] = (gcb[k] + gcr[k]).astype(BF16)
            for who in range(2):
                pltpu.make_async_copy(
                    gcv.at[k, who],
                    gc_hbm.at[pl.ds(who * TH, TH), pl.ds(k * QR, QR)],
                    o_sem.at[4],
                ).start()

    steps_z = NZ // 2
    NK = H // QR
    per = max(1, NK // 2)
    stages = [(x_start, 0), (z_sum, 6), (x_second, 3), (x_first, 1)]
    z_stages = [z_start]
    z_stages += [lambda i, n=n: z_ring(i)[1](n) for n in range(2, steps_z + 1)]
    z_stages += [z_last, x_sum]
    gain_steps = (2, 3, NB - 1, NB + 2, NB + 5)
    last = max([NB + 6] + [b + Z_PLAN[b][steps_z + 1] + 1 for b in ZB])

    def step(t):
        for stage, lag in stages:
            mine = (t >= lag) & (t < NB + lag)
            if stage is x_second:
                mine = mine & (t != NB - 1 + lag)
            for b in ZB:
                mine = mine & (t != b + lag)

            @pl.when(mine)
            def _():
                with jax.named_scope(stage.__name__):
                    stage(t - lag)

        @pl.when(t == NB + 1)
        def _():
            with jax.named_scope("x_second_last"):
                x_second(NB - 1)

        for n, stage in enumerate(z_stages):
            for i, b in enumerate(ZB):

                @pl.when(t == b + Z_PLAN[b][n])
                def _():
                    with jax.named_scope(f"z{n}#b={b}"):
                        stage(i)

        for k, when in enumerate(gain_steps):

            @pl.when(t == when)
            def _():
                with jax.named_scope("gain_stage"):
                    gain_stage(k)

        @pl.when((t >= NB) & (t < NB + NK // per))
        def _():
            with jax.named_scope("context_grad"):
                each_block(per, lambda i: context_grad((t - NB) * per + i))

        @pl.when(t == NB + 2)
        def _():
            with jax.named_scope("context_join"):
                context_join()

    with jax.named_scope("context_own"):
        each_block(NK, context_own)
    each_block(last, step)

    gain_out = pltpu.make_async_copy(gg_ref, gg_hbm, o_sem.at[0])
    gain_out.start()
    ctx_swap().wait_send()
    landed(psend, p_s.at[0])
    for hop in hops:
        if hop[3] > 1:
            landed(hop[0].at[pl.ds(0, hop[3] - 1)], hop[4])

    landed(gaf.at[:, :, m], ga_s.at[0])
    landed(gaf.at[0, :, m], sa_s.at[0])
    landed(gcs, gc_s.at[0])
    landed(fs.at[oc], f_s.at[0])

    def drain(j):
        for r in range(2):
            x_ring(j, r)[3]()
        landed(zr.at[j, pl.ds(1, ZY - 1)], z_s.at[j])

    for j in range(NB):
        if j not in ZB:
            drain(j)
    for i in range(len(ZB)):
        z_ring(i)[3]()
        landed(xr.at[i, pl.ds(1, NX * NY - 1)], xo_s.at[i])
    landed(gcv, o_sem.at[4])
    with jax.named_scope("core_wait"):
        landed(g_hbm.at[oc], f_r.at[0])

    landed(g_hbm.at[c], o_sem.at[1])
    gain_out.wait()


def deliver(
    dims,
    g_hbm, gg_hbm, gc_hbm, w_hbm, m1_hbm, m2_hbm,
    nw_hbm, n1_hbm, n2_hbm, gg_out, gc_out,
    gv, ggv, gcv, w16, m1v, m2v, nwv, n1v, n2v, sem,
):
    NZ, NY, NX, TH, H, D, NB, CB = dims
    z, yl, x, c = (lax.axis_index(a) for a in DP)
    row = pl.multiple_of(((z * NY + yl) * NX + x) * 16, 16)
    pairs = [(gc_hbm, gcv), (gg_hbm, ggv), (g_hbm, gv), (w_hbm.at[pl.ds(row, 16), :], w16), (m1_hbm, m1v), (m2_hbm, m2v)]
    into = [pltpu.make_async_copy(a, b, sem.at[i]) for i, (a, b) in enumerate(pairs)]
    pairs = [(gcv, gc_out), (ggv, gg_out), (nwv, nw_hbm), (n1v, n1_hbm), (n2v, n2_hbm)]
    out = [pltpu.make_async_copy(a, b, sem.at[6 + i]) for i, (a, b) in enumerate(pairs)]
    for copy in into:
        copy.start()
    for i in range(2):
        into[i].wait()
        out[i].start()
    for copy in into[2:]:
        copy.wait()
    for b in range(2 * NB):
        cols = slice(b * CB, (b + 1) * CB)
        g = gv[b // NB, b % NB]
        first = beta_one * m1v[:, cols] + (1.0 - beta_one) * g
        second = beta_two * m2v[:, cols] + (1.0 - beta_two) * g * g
        both = w16[:, cols].astype(F32)
        master = jnp.where(c == 0, both[:8], both[8:])
        n1v[:, cols] = first
        n2v[:, cols] = second
        nwv[:, cols] = (master - learn_rate * first / (jnp.sqrt(second) + adam_floor)).astype(BF16)
    for copy in out[2:]:
        copy.start()
    for copy in out:
        copy.wait()


def per_device(sizes, block, context, out_weight, cotangent, norm_gain, first_moment, second_moment):
    NZ, NY, NX = sizes
    T, H = context.shape
    D = out_weight.shape[1]
    TH, CB = T // 2, block
    NB = D // (2 * CB)
    NB2 = 2 * NB
    ZY = NZ * NY
    NZB = len(z_blocks(NB))
    rows8 = (NB2 + 7) // 8 * 8
    dims = (NZ, NY, NX, TH, H, D, NB, CB)
    dma = pltpu.SemaphoreType.DMA
    scratch = [
        pltpu.VMEM((D,), F32),
        pltpu.VMEM((H // QR, 2, TH, QR), BF16),
        pltpu.VMEM((H // QR, TH, QR), F32),
        pltpu.VMEM((H // QR, TH, QR), F32),
        pltpu.VMEM((H // QR, TH, QR), F32),
        pltpu.VMEM((2, TH, H), BF16),
        pltpu.VMEM((2, TH, H), BF16),
        pltpu.VMEM((NB2, H, CB), BF16),
        pltpu.VMEM((TH, D), BF16),
        pltpu.VMEM((NB2, TH, CB), F32),
        pltpu.VMEM((NB2, TH, CB), BF16),
        pltpu.VMEM((NB2, TH, CB), BF16),
        pltpu.VMEM((TH, 128), F32),
        pltpu.VMEM((TH, 128), F32),
        pltpu.VMEM((2, NB, 2, TH, CB), BF16),
        pltpu.VMEM((NB, 2, TH, CB), BF16),
        pltpu.VMEM((NB, NZ * NY * NX, 16, CB), F32),
        pltpu.VMEM((NB, max(ZY, NY * NX), 16, CB), F32),
        pltpu.VMEM((NB, 2, (NX - 1) * NZ, 16, CB), BF16),
        pltpu.VMEM((NZB, (NZ - 1) * NY * NX, 16, CB), BF16),
        pltpu.VMEM((NB, 2, NX // 2, 2, NZ, 16, CB), BF16),
        pltpu.VMEM((NZB, NZ // 2, 2, NY * NX, 16, CB), BF16),
        pltpu.VMEM((NB, NY, NZ, 16, CB), BF16),
        pltpu.VMEM((NB, ZY, 16, CB), BF16),
        pltpu.VMEM((NZB, NY, NX, 16, CB), BF16),
        pltpu.VMEM((NZB, NX * NY, 16, CB), BF16),
        pltpu.VMEM((2, NB, 8, CB), F32),
        pltpu.VMEM((NZ, rows8, CB), F32),
        pltpu.VMEM((NX, rows8, CB), F32),
        pltpu.VMEM((NY, rows8, CB), F32),
        pltpu.VMEM((2, rows8, CB), F32),
        pltpu.VMEM((2, rows8, CB), F32),
        dma((NB2,)), dma((5,)), dma((2,)),
        dma((1,)), dma((NB2 + 1,)),
        dma((1,)), dma((NB,)),
        dma((1,)), dma((NB,)),
        dma((NB, 2)), dma((NB, 2, NX // 2)),
        dma((NZB,)), dma((NZB, NZ // 2)),
        dma((NB,)), dma((NB,)),
        dma((NZB,)), dma((NZB,)),
        dma((5,)),
        dma((1,)), dma((1,)),
        dma((5,)), dma((5,)),
        dma((2,)),
    ]
    any_space = pl.BlockSpec(memory_space=pl.ANY)
    vmem = pl.BlockSpec(memory_space=pltpu.VMEM)
    g, gg, gc = pl.pallas_call(
        functools.partial(kernel, dims),
        out_shape=[
            jax.ShapeDtypeStruct((2, NB, 8, CB), F32),
            jax.ShapeDtypeStruct((D,), F32),
            jax.ShapeDtypeStruct((T, H), BF16),
        ],
        in_specs=[any_space, any_space, any_space, vmem],
        out_specs=[any_space] * 3,
        scratch_shapes=scratch,
        compiler_params=pltpu.CompilerParams(
            collective_id=0, has_side_effects=True, vmem_limit_bytes=60 * 1024 * 1024
        ),
        name="step",
    )(context, out_weight, cotangent, norm_gain)
    shard = jax.ShapeDtypeStruct((8, D), F32)
    results = [jax.ShapeDtypeStruct((8, D), BF16), shard, shard, jax.ShapeDtypeStruct((D,), F32)]
    results.append(jax.ShapeDtypeStruct((T, H), BF16))
    moved = [(2, NB, 8, CB), (D,), (T, H), (16, D), (8, D), (8, D), (8, D), (8, D), (8, D)]
    types = [F32, F32, BF16, BF16, F32, F32, BF16, F32, F32]
    nw, n1, n2, gg, gc = pl.pallas_call(
        functools.partial(deliver, dims),
        out_shape=results,
        in_specs=[any_space] * 6,
        out_specs=[any_space] * 5,
        scratch_shapes=[pltpu.VMEM(a, b) for a, b in zip(moved, types)] + [dma((11,))],
        compiler_params=pltpu.CompilerParams(vmem_limit_bytes=60 * 1024 * 1024),
        name="deliver",
    )(g, gg, gc, out_weight, first_moment[0], second_moment[0])
    return (nw[None], n1[None], n2[None], gg, gc)


def build(finer, block):
    sizes = tuple(finer.shape[a] for a in ("dp_0", "dp_1", "dp_2"))
    placed = (P(DP, "mp"), P("mp", None), P(DP, None), P(), P("mp", DP, None), P("mp", DP, None))
    return jax.shard_map(
        functools.partial(per_device, sizes, block),
        mesh=finer,
        in_specs=placed,
        out_specs=(P("mp", DP, None), P("mp", DP, None), P("mp", DP, None), P(), P(DP, "mp")),
        check_vma=False,
    )


def solution(mesh):
    finer = Mesh(
        mesh.devices.reshape(8, 2, 4, 2, mesh.shape["mp"]), ("dp_0", "dp_1", "dp_2", "dp_3", "mp")
    )
    return build(finer, 256)
```
